32 devices in a mesh: gx: 16 (over z, y, x), gy: 1, gz: 2 (over core).
Axes of the slice: x: 2, y: 2, z: 4, core: 2. Of those that a mesh axis runs over, the one named last changes fastest.
Arguments:
- populations: float32 [19, 128, 8, 256], P(None, 'gx', 'gy', 'gz'), may hold values from 0.01 to 0.11
Outputs:
- populations_next: float32 [19, 128, 8, 256], P(None, 'gx', 'gy', 'gz')
- moments_slab: float32 [4, 256, 8, 128], P(None, ('gz', 'gx'), 'gy')
The draws below stay inside these ranges and needn't reach their ends.
All inputs are finite; a program needn't handle non-finite values.
Results may differ from the reference program's by a relative error of at most 0.0003.
Values sent between devices are 32-bit elements; how exact they have to be, the bound alone decides.
A program may use at most 64 MiB of HBM per device.

```python
from functools import reduce
import jax
import jax.numpy as jnp

Q = 19
NX = 128
NY = 8
NZ = 256


def levels(key, dims, cuts, least, largest):
    loudness = 1.0
    for position, parts in cuts:
        heights = jax.random.uniform(jax.random.fold_in(jax.random.fold_in(key, 6), position), (parts,), jnp.float32, least / len(cuts), largest / len(cuts))
        loudness = loudness * jnp.repeat(jnp.exp(heights), dims[position] // parts).reshape((-1,) + (1,) * (len(dims) - 1 - position))
    return loudness


def setup_inputs(seed: int = 0) -> dict:
    seeds = jax.random.split(jax.random.key(seed), 2)
    populations = jnp.clip(0.01 + 0.1 * jax.random.uniform(seeds[0], (Q, NX, NY, NZ), jnp.float32) ** levels(seeds[0], (Q, NX, NY, NZ), ((1, 16), (3, 2)), -0.2, 0.2), 0.01, 0.11)
    return dict(populations=populations)


lattice_moves = [(0, 0, 0), (1, 0, 0), (-1, 0, 0), (0, 1, 0), (0, -1, 0), (0, 0, 1), (0, 0, -1),
                 (1, 1, 0), (-1, -1, 0), (1, -1, 0), (-1, 1, 0), (1, 0, 1), (-1, 0, -1), (1, 0, -1), (-1, 0, 1),
                 (0, 1, 1), (0, -1, -1), (0, 1, -1), (0, -1, 1)]
lattice_weights = [1.0 / 3.0] + [1.0 / 18.0] * 6 + [1.0 / 36.0] * 12
relaxation = 1.6


def signed_total(pieces, component):
    total = jnp.zeros_like(pieces[0])
    for move, piece in zip(lattice_moves, pieces):
        if move[component] == 1:
            total = total + piece
        elif move[component] == -1:
            total = total - piece
    return total


def lattice_moments(pieces):
    density = reduce(lambda left, right: left + right, pieces)
    velocity_x = signed_total(pieces, 0) / density
    velocity_y = signed_total(pieces, 1) / density
    velocity_z = signed_total(pieces, 2) / density
    return density, velocity_x, velocity_y, velocity_z


def collide(pieces):
    density, velocity_x, velocity_y, velocity_z = lattice_moments(pieces)
    speed_sq = velocity_x * velocity_x + velocity_y * velocity_y + velocity_z * velocity_z
    result = []
    for move, weight, piece in zip(lattice_moves, lattice_weights, pieces):
        projected = move[0] * velocity_x + move[1] * velocity_y + move[2] * velocity_z
        balance = weight * density * (1.0 + 3.0 * projected + 4.5 * projected * projected - 1.5 * speed_sq)
        result.append(piece - relaxation * (piece - balance))
    return result


def reference(populations):
    pieces = [populations[index] for index in range(19)]
    moments = jnp.stack(lattice_moments(pieces))
    moments_slab = jnp.transpose(moments, (0, 3, 2, 1))
    read = [jnp.roll(pieces[index], lattice_moves[index], axis=(0, 1, 2)) for index in range(19)]
    populations_next = jnp.stack(collide(read))
    return populations_next, moments_slab
```

```python
import functools

import jax
import jax.numpy as jnp
from jax import lax
from jax.experimental import pallas as pl
from jax.experimental.pallas import tpu as pltpu
from jax.sharding import PartitionSpec as P

MESH = pl.DeviceIdType.MESH

lattice_moves = [
    (0, 0, 0),
    (1, 0, 0),
    (-1, 0, 0),
    (0, 1, 0),
    (0, -1, 0),
    (0, 0, 1),
    (0, 0, -1),
    (1, 1, 0),
    (-1, -1, 0),
    (1, -1, 0),
    (-1, 1, 0),
    (1, 0, 1),
    (-1, 0, -1),
    (1, 0, -1),
    (-1, 0, 1),
    (0, 1, 1),
    (0, -1, -1),
    (0, 1, -1),
    (0, -1, 1),
]
lattice_weights = [1.0 / 3.0] + [1.0 / 18.0] * 6 + [1.0 / 36.0] * 12
relaxation = 1.6
count_q = len(lattice_moves)


def movers(component, sign):
    return [q for q, move in enumerate(lattice_moves) if move[component] == sign]


def place_in(q, component):
    return movers(component, lattice_moves[q][component]).index(q)


def side(sign):
    return 0 if sign > 0 else 1


edges_xz = [q for q, m in enumerate(lattice_moves) if m[0] and m[2]]
edges_xy = [q for q, m in enumerate(lattice_moves) if m[0] and m[1]]
edges_yz = [q for q, m in enumerate(lattice_moves) if m[1] and m[2]]


def total(terms):
    terms = list(terms)
    while len(terms) > 1:
        terms = [
            terms[i] + terms[i + 1] if i + 1 < len(terms) else terms[i]
            for i in range(0, len(terms), 2)
        ]
    return terms[0]


def moments_of(f):
    density = total(f)
    inverse = 1.0 / density
    velocity = []
    for component in range(3):
        plus = total(f[q] for q in movers(component, 1))
        minus = total(f[q] for q in movers(component, -1))
        velocity.append((plus - minus) * inverse)
    return density, velocity


def collided(f):
    density, velocity = moments_of(f)
    speed_sq = velocity[0] * velocity[0] + velocity[1] * velocity[1] + velocity[2] * velocity[2]
    base = 1.0 - 1.5 * speed_sq
    scaled = {w: (relaxation * w) * density for w in set(lattice_weights)}
    keep = 1.0 - relaxation
    result = [None] * count_q
    result[0] = keep * f[0] + scaled[lattice_weights[0]] * base
    for q in range(1, count_q, 2):
        move = lattice_moves[q]
        projected = None
        for component in range(3):
            if move[component] == 0:
                continue
            if projected is None:
                projected = velocity[component] if move[component] > 0 else -velocity[component]
            elif move[component] > 0:
                projected = projected + velocity[component]
            else:
                projected = projected - velocity[component]
        even = base + 4.5 * (projected * projected)
        odd = 3.0 * projected
        weight = scaled[lattice_weights[q]]
        result[q] = keep * f[q] + weight * (even + odd)
        result[q + 1] = keep * f[q + 1] + weight * (even - odd)
    return result


def rolled(v, shift, axis):
    return pltpu.roll(v, shift % v.shape[axis], axis)


load_chunks = ((0, 4), (4, 8))


def kernel(axes, sizes, pop_hbm, out_vm, recv_m,
           pop, land_x, face_z, pack_x, pack_z, send_m,
           row_y, face_y, edge_xy, edge_yz,
           load_sem, send_sem, recv_sem, *y_sems):
    nx, ny, nz = (sizes[a] for a in axes)
    here = tuple(lax.axis_index(a) for a in axes)
    _, lx, ly, lz = pop.shape
    split_y = ny > 1
    faces = 2 * len(movers(0, 1))

    def device_at(offset):
        return tuple(
            lax.rem(h + o % n, n) if o % n else h
            for h, o, n in zip(here, offset, (nx, ny, nz))
        )

    loads = []
    for i, (first, last) in enumerate(load_chunks):
        planes = pl.ds(first * lx // 8, (last - first) * lx // 8)
        load = pltpu.make_async_copy(pop_hbm.at[:, planes], pop.at[:, planes], load_sem.at[i])
        load.start()
        loads.append(load)

    offsets = [(k, 0, 0) for k in range(1, nx)]
    offsets += [(0, 0, 1), (0, 0, -1)]
    offsets += [lattice_moves[q] for q in edges_xz]
    if split_y:
        offsets += [(0, 1, 0), (0, -1, 0)]
        offsets += [lattice_moves[q] for q in edges_xy + edges_yz]
    partners = sorted({(a % nx, b % ny, c % nz) for a, b, c in offsets})
    barrier = pltpu.get_barrier_semaphore()
    for offset in partners:
        pl.semaphore_signal(barrier, inc=1, device_id=device_at(offset), device_id_type=MESH)

    lane = lax.broadcasted_iota(jnp.int32, (ly, lz), 1)
    row = lax.broadcasted_iota(jnp.int32, (ly, lz), 0)

    def remote(src, dst, sem, offset):
        return pltpu.make_async_remote_copy(
            src_ref=src, dst_ref=dst, send_sem=send_sem.at[sem], recv_sem=recv_sem.at[sem],
            device_id=device_at(offset), device_id_type=MESH)

    y_copies = []

    def send_y(src, dst, offset):
        s = len(y_copies)
        copy = pltpu.make_async_remote_copy(
            src_ref=src, dst_ref=dst, send_sem=y_sems[0].at[s], recv_sem=y_sems[1].at[s],
            device_id=device_at(offset), device_id_type=MESH)
        copy.start()
        y_copies.append(copy)

    lane_x = lane & (lx - 1)
    turned = [[None] * lx for _ in range(4)]

    def measure(x):
        density, velocity = moments_of([pop[q, x] for q in range(count_q)])
        for c, value in enumerate([density] + velocity):
            for z in range(lx):
                moved = rolled(value, x - z, 1) if x != z else value
                turned[c][z] = moved if turned[c][z] is None else jnp.where(lane_x == x, moved, turned[c][z])

    for i, (first, last) in enumerate(load_chunks):
        loads[i].wait()
        if i == len(load_chunks) - 1:
            for sign in (1, -1):
                at = lx - 1 if sign > 0 else 0
                up, down = (lattice_moves.index((sign, 0, cz)) for cz in (1, -1))
                pack_x[side(sign)] = jnp.where(lane == lz - 1, pop[up, at], pop[down, at])
            pl.semaphore_wait(barrier, len(partners))
            for sign in (1, -1):
                s, at = side(sign), lx - 1 if sign > 0 else 0
                for j, q in enumerate(movers(0, sign)):
                    remote(pop.at[q, at], land_x.at[s * faces // 2 + j], 0, (sign, 0, 0)).start()
            edge_slot = {}
            for q in edges_xz:
                cx, _, cz = lattice_moves[q]
                if (cx, cz % nz) not in edge_slot:
                    edge_slot[cx, cz % nz] = faces + len(edge_slot)
                    remote(pack_x.at[side(cx)], land_x.at[edge_slot[cx, cz % nz]], 0, lattice_moves[q]).start()
        for x in range(first * lx // 8, last * lx // 8):
            measure(x)

    for p in range(2):
        square = jnp.concatenate(turned[2 * p] + turned[2 * p + 1], axis=0).T
        for j in range(nx):
            send_m[j, p] = square[j * lx:(j + 1) * lx]

    me = here[0]
    for k in range(1, nx):
        target = lax.rem(me + k, nx)
        remote(send_m.at[target], recv_m.at[me], 2, (k, 0, 0)).start()

    for sign in (1, -1):
        at = lz - 1 if sign > 0 else 0
        packed = jnp.zeros((ly, lz), jnp.float32)
        for i, q in enumerate(movers(2, sign)):
            for x in range(lx):
                k = i * lx + x
                packed = jnp.where(lane == k, rolled(pop[q, x], k - at, 1), packed)
        pack_z[side(sign)] = packed
    for sign in (1, -1):
        s = side(sign)
        remote(pack_z.at[s], face_z.at[s], 1, (0, 0, sign)).start()
    if split_y:
        for sign in (1, -1):
            at = ly - 1 if sign > 0 else 0
            for i, q in enumerate(movers(1, sign)):
                for x in range(lx):
                    row_y[side(sign), i, x:x + 1, :] = pop[q, x, at:at + 1, :]
        for sign in (1, -1):
            s = side(sign)
            send_y(row_y.at[s], face_y.at[s], (0, sign, 0))
        for i, q in enumerate(edges_yz):
            s = side(lattice_moves[q][2])
            send_y(pack_z.at[s], edge_yz.at[i], lattice_moves[q])
        for i, q in enumerate(edges_xy):
            s = side(lattice_moves[q][1])
            send_y(row_y.at[s, place_in(q, 1)], edge_xy.at[i], lattice_moves[q])
    recv_m[me] = send_m[me]

    all_x = remote(land_x, land_x, 0, (1, 0, 0))
    all_z = remote(face_z, face_z, 1, (0, 0, 1))
    others = pl.ds(0, nx - 1)
    all_m = remote(send_m.at[others], send_m.at[others], 2, (1, 0, 0))

    def streamed(q, x):
        cx, cy, cz = lattice_moves[q]
        sx = x - cx
        inside = 0 <= sx < lx
        sx_wrapped = sx % lx
        v = pop[q, sx] if inside else land_x[side(cx) * faces // 2 + place_in(q, 0)]
        if cy and split_y:
            at = ly - 1 if cy > 0 else 0
            if inside:
                other = face_y[side(cy), place_in(q, 1), sx:sx + 1, :]
            else:
                other = edge_xy[edges_xy.index(q), sx_wrapped:sx_wrapped + 1, :]
            v = jnp.where(row == at, jnp.broadcast_to(other, v.shape), v)
        if cz:
            at = lz - 1 if cz > 0 else 0
            if inside:
                other = face_z[side(cz)]
                if cy and split_y:
                    at_y = ly - 1 if cy > 0 else 0
                    other = jnp.where(row == at_y, edge_yz[edges_yz.index(q)], other)
                k = place_in(q, 2) * lx + sx
                other = rolled(other, at - k, 1)
            else:
                other = land_x[edge_slot[cx, cz % nz]]
            v = jnp.where(lane == at, other, v)
        if cy:
            v = rolled(v, cy, 0)
        if cz:
            v = rolled(v, cz, 1)
        return v

    def advance(x):
        result = collided([streamed(q, x) for q in range(count_q)])
        for q in range(count_q):
            out_vm[q, x] = result[q]

    all_z.wait_recv()
    for copy in y_copies:
        copy.wait_recv()
    for x in range(1, lx - 1):
        advance(x)
    all_x.wait_recv()
    advance(0)
    advance(lx - 1)

    for copy in [all_x, all_z, all_m] + y_copies:
        copy.wait_send()
    all_m.wait_recv()


def finish(next_vm, recv_m, next_ref, slab_ref, slab_vm, sems):
    store = pltpu.make_async_copy(next_vm, next_ref, sems.at[0])
    store.start()
    _, lx, ly, lz = slab_vm.shape
    for p in range(2):
        square = recv_m[:, p].reshape(lz, lz).T
        slab_vm[2 * p:2 * p + 2] = square.reshape(2, lx, ly, lz)
    slab_store = pltpu.make_async_copy(slab_vm, slab_ref, sems.at[1])
    slab_store.start()
    store.wait()
    slab_store.wait()


def on_device(axes, sizes, populations):
    q, lx, ly, lz = populations.shape
    nx, ny, nz = (sizes[a] for a in axes)
    faces = 2 * len(movers(0, 1))
    edges = 4 if nz > 2 else 2
    f32 = jnp.float32
    tile = (ly, lz)
    y_sems = [pltpu.SemaphoreType.DMA((10,))] * 2 if ny > 1 else []
    held = pl.pallas_call(
        functools.partial(kernel, axes, sizes),
        out_shape=(
            pltpu.VMEM(populations.shape, f32),
            pltpu.VMEM((nx, 2, lx, lz), f32),
        ),
        in_specs=[pl.BlockSpec(memory_space=pl.ANY)],
        out_specs=(pl.BlockSpec(memory_space=pltpu.VMEM),) * 2,
        scratch_shapes=[
            pltpu.VMEM(populations.shape, f32),
            pltpu.VMEM((faces + edges,) + tile, f32),
            pltpu.VMEM((2,) + tile, f32),
            pltpu.VMEM((2,) + tile, f32),
            pltpu.VMEM((2,) + tile, f32),
            pltpu.VMEM((nx, 2, lx, lz), f32),
            pltpu.VMEM((2, 5, lx, lz), f32),
            pltpu.VMEM((2, 5, lx, lz), f32),
            pltpu.VMEM((4, lx, lz), f32),
            pltpu.VMEM((4,) + tile, f32),
            pltpu.SemaphoreType.DMA((len(load_chunks),)),
            pltpu.SemaphoreType.DMA((3,)),
            pltpu.SemaphoreType.DMA((3,)),
        ] + y_sems,
        compiler_params=pltpu.CompilerParams(collective_id=0, has_side_effects=True),
        name="lattice_step",
    )(populations)
    held = [pltpu.with_memory_space_constraint(h, pltpu.VMEM) for h in held]
    slab = (4, lx, ly, lz)
    return pl.pallas_call(
        finish,
        out_shape=(jax.ShapeDtypeStruct(populations.shape, f32), jax.ShapeDtypeStruct(slab, f32)),
        in_specs=[pl.BlockSpec(memory_space=pltpu.VMEM)] * 2,
        out_specs=(pl.BlockSpec(memory_space=pl.ANY),) * 2,
        scratch_shapes=[pltpu.VMEM(slab, f32), pltpu.SemaphoreType.DMA((2,))],
        name="finish",
    )(*held)


def solution(mesh):
    axes = tuple(mesh.axis_names)
    sizes = dict(mesh.shape)
    return jax.shard_map(
        functools.partial(on_device, axes, sizes),
        mesh=mesh,
        in_specs=(P(None, "gx", "gy", "gz"),),
        out_specs=(P(None, "gx", "gy", "gz"), P(None, ("gz", "gx"), "gy", None)),
        check_vma=False,
    )
```

```python
import functools

import jax
import jax.numpy as jnp
from jax import lax
from jax.experimental import pallas as pl
from jax.experimental.pallas import tpu as pltpu
from jax.sharding import PartitionSpec as P

MESH = pl.DeviceIdType.MESH

lattice_moves = [
    (0, 0, 0),
    (1, 0, 0),
    (-1, 0, 0),
    (0, 1, 0),
    (0, -1, 0),
    (0, 0, 1),
    (0, 0, -1),
    (1, 1, 0),
    (-1, -1, 0),
    (1, -1, 0),
    (-1, 1, 0),
    (1, 0, 1),
    (-1, 0, -1),
    (1, 0, -1),
    (-1, 0, 1),
    (0, 1, 1),
    (0, -1, -1),
    (0, 1, -1),
    (0, -1, 1),
]
lattice_weights = [1.0 / 3.0] + [1.0 / 18.0] * 6 + [1.0 / 36.0] * 12
relaxation = 1.6
count_q = len(lattice_moves)


def movers(component, sign):
    return [q for q, move in enumerate(lattice_moves) if move[component] == sign]


def place_in(q, component):
    return movers(component, lattice_moves[q][component]).index(q)


def side(sign):
    return 0 if sign > 0 else 1


edges_xz = [q for q, m in enumerate(lattice_moves) if m[0] and m[2]]
edges_xy = [q for q, m in enumerate(lattice_moves) if m[0] and m[1]]
edges_yz = [q for q, m in enumerate(lattice_moves) if m[1] and m[2]]


def total(terms):
    terms = list(terms)
    while len(terms) > 1:
        terms = [
            terms[i] + terms[i + 1] if i + 1 < len(terms) else terms[i]
            for i in range(0, len(terms), 2)
        ]
    return terms[0]


def moments_of(f):
    density = total(f)
    inverse = 1.0 / density
    velocity = []
    for component in range(3):
        plus = total(f[q] for q in movers(component, 1))
        minus = total(f[q] for q in movers(component, -1))
        velocity.append((plus - minus) * inverse)
    return density, velocity


def collided(f):
    density, velocity = moments_of(f)
    speed_sq = velocity[0] * velocity[0] + velocity[1] * velocity[1] + velocity[2] * velocity[2]
    base = 1.0 - 1.5 * speed_sq
    scaled = {w: (relaxation * w) * density for w in set(lattice_weights)}
    keep = 1.0 - relaxation
    result = [None] * count_q
    result[0] = keep * f[0] + scaled[lattice_weights[0]] * base
    for q in range(1, count_q, 2):
        move = lattice_moves[q]
        projected = None
        for component in range(3):
            if move[component] == 0:
                continue
            if projected is None:
                projected = velocity[component] if move[component] > 0 else -velocity[component]
            elif move[component] > 0:
                projected = projected + velocity[component]
            else:
                projected = projected - velocity[component]
        even = base + 4.5 * (projected * projected)
        odd = 3.0 * projected
        weight = scaled[lattice_weights[q]]
        result[q] = keep * f[q] + weight * (even + odd)
        result[q + 1] = keep * f[q + 1] + weight * (even - odd)
    return result


def rolled(v, shift, axis):
    return pltpu.roll(v, shift % v.shape[axis], axis)


load_chunks = ((0, 4), (4, 8))
ack_groups = 4


def kernel(axes, sizes, pop_hbm, out_vm, recv_m,
           pop, land_x, face_z, pack_x, pack_z, send_m,
           row_y, face_y, edge_xy, edge_yz,
           load_sem, send_sem, recv_sem, ack_sem, *y_sems):
    nx, ny, nz = (sizes[a] for a in axes)
    here = tuple(lax.axis_index(a) for a in axes)
    _, lx, ly, lz = pop.shape
    split_y = ny > 1
    faces = 2 * len(movers(0, 1))

    def device_at(offset):
        return tuple(
            lax.rem(h + o % n, n) if o % n else h
            for h, o, n in zip(here, offset, (nx, ny, nz))
        )

    loads = []
    for i, (first, last) in enumerate(load_chunks):
        planes = pl.ds(first * lx // 8, (last - first) * lx // 8)
        load = pltpu.make_async_copy(pop_hbm.at[:, planes], pop.at[:, planes], load_sem.at[i])
        load.start()
        loads.append(load)

    offsets = [(k, 0, 0) for k in range(1, nx)]
    offsets += [(0, 0, 1), (0, 0, -1)]
    offsets += [lattice_moves[q] for q in edges_xz]
    if split_y:
        offsets += [(0, 1, 0), (0, -1, 0)]
        offsets += [lattice_moves[q] for q in edges_xy + edges_yz]
    partners = sorted({(a % nx, b % ny, c % nz) for a, b, c in offsets})
    around = [o for o in partners if o[1] or o[2]]
    me = here[0]
    rank = (me * ny + here[1]) * nz + here[2]

    def rank_of(offset):
        a, b, c = device_at(offset)
        return (a * ny + b) * nz + c

    span = -(-nx // ack_groups)

    def column(target):
        return (target,) + here[1:]

    barrier = pltpu.get_barrier_semaphore()

    def wait_some(sem, count):
        @pl.when(count > 0)
        def _():
            pl.semaphore_wait(sem, count)

    acks = ack_sem.at[1 + me // span]

    def announce(target, carry):
        pl.semaphore_signal(barrier, inc=1, device_id=column(target), device_id_type=MESH)
        return carry

    def acknowledge(target, carry):
        pl.semaphore_signal(acks, inc=1, device_id=column(target), device_id_type=MESH)
        return carry

    lower = me
    higher_z = jnp.int32(0)
    higher_around = []
    for offset in around:
        @pl.when(rank_of(offset) > rank)
        def _():
            pl.semaphore_signal(barrier, inc=1, device_id=device_at(offset), device_id_type=MESH)

        lower = lower + jnp.where(rank_of(offset) < rank, 1, 0)
        above = jnp.where(rank_of(offset) > rank, 1, 0)
        if offset[0] == offset[1] == 0:
            higher_z = higher_z + above
        else:
            higher_around.append((device_at(offset)[0] // span, above))
    lax.fori_loop(me + 1, nx, announce, 0)
    wait_some(barrier, lower)
    for offset in around:
        @pl.when(rank_of(offset) < rank)
        def _():
            pl.semaphore_signal(
                ack_sem.at[0] if offset[0] == offset[1] == 0 else acks, inc=1,
                device_id=device_at(offset), device_id_type=MESH)
    lax.fori_loop(0, me, acknowledge, 0)

    lane = lax.broadcasted_iota(jnp.int32, (ly, lz), 1)
    row = lax.broadcasted_iota(jnp.int32, (ly, lz), 0)

    def remote(src, dst, sem, offset):
        return pltpu.make_async_remote_copy(
            src_ref=src, dst_ref=dst, send_sem=send_sem.at[sem], recv_sem=recv_sem.at[sem],
            device_id=device_at(offset), device_id_type=MESH)

    y_copies = []

    def send_y(src, dst, offset):
        s = len(y_copies)
        copy = pltpu.make_async_remote_copy(
            src_ref=src, dst_ref=dst, send_sem=y_sems[0].at[s], recv_sem=y_sems[1].at[s],
            device_id=device_at(offset), device_id_type=MESH)
        copy.start()
        y_copies.append(copy)

    lane_x = lane & (lx - 1)
    turned = [[None] * lx for _ in range(4)]

    def measure(x):
        density, velocity = moments_of([pop[q, x] for q in range(count_q)])
        for c, value in enumerate([density] + velocity):
            for z in range(lx):
                moved = rolled(value, x - z, 1) if x != z else value
                turned[c][z] = moved if turned[c][z] is None else jnp.where(lane_x == x, moved, turned[c][z])

    edge_slot = {}
    for q in edges_xz:
        cx, _, cz = lattice_moves[q]
        edge_slot.setdefault((cx, cz % nz), faces + len(edge_slot))

    def send_faces(chosen):
        for sign in (1, -1):
            @pl.when(chosen((sign, 0, 0)))
            def _():
                s, at = side(sign), lx - 1 if sign > 0 else 0
                for j, q in enumerate(movers(0, sign)):
                    remote(pop.at[q, at], land_x.at[s * faces // 2 + j], 0, (sign, 0, 0)).start()
                for (cx, cz), slot in edge_slot.items():
                    if cx == sign:
                        remote(pack_x.at[s], land_x.at[slot], 0, (cx, 0, cz)).start()

    def send_moments(target):
        pltpu.make_async_remote_copy(
            src_ref=send_m.at[target], dst_ref=recv_m.at[me],
            send_sem=send_sem.at[2], recv_sem=recv_sem.at[2],
            device_id=column(target), device_id_type=MESH).start()

    def send_each(target, carry):
        send_moments(target)
        return carry

    def send_z(sign):
        remote(pack_z.at[side(sign)], face_z.at[side(sign)], 1, (0, 0, sign)).start()

    for i, (first, last) in enumerate(load_chunks):
        loads[i].wait()
        if i == len(load_chunks) - 1:
            for sign in (1, -1):
                at = lx - 1 if sign > 0 else 0
                up, down = (lattice_moves.index((sign, 0, cz)) for cz in (1, -1))
                pack_x[side(sign)] = jnp.where(lane == lz - 1, pop[up, at], pop[down, at])
            send_faces(lambda offset: rank_of(offset) < rank)
        for x in range(first * lx // 8, last * lx // 8):
            measure(x)

    for p in range(2):
        square = jnp.concatenate(turned[2 * p] + turned[2 * p + 1], axis=0).T
        for j in range(nx):
            send_m[j, p] = square[j * lx:(j + 1) * lx]

    lax.fori_loop(0, me, send_each, 0)

    for sign in (1, -1):
        at = lz - 1 if sign > 0 else 0
        packed = jnp.zeros((ly, lz), jnp.float32)
        for i, q in enumerate(movers(2, sign)):
            for x in range(lx):
                k = i * lx + x
                packed = jnp.where(lane == k, rolled(pop[q, x], k - at, 1), packed)
        pack_z[side(sign)] = packed
    for sign in (1, -1):
        @pl.when(rank_of((0, 0, sign)) < rank)
        def _():
            send_z(sign)

    wait_some(ack_sem.at[0], higher_z)
    for sign in (1, -1):
        @pl.when(rank_of((0, 0, sign)) > rank)
        def _():
            send_z(sign)

    recv_m[me] = send_m[me]

    all_x = remote(land_x, land_x, 0, (1, 0, 0))
    all_z = remote(face_z, face_z, 1, (0, 0, 1))
    others = pl.ds(0, nx - 1)
    all_m = remote(send_m.at[others], send_m.at[others], 2, (1, 0, 0))

    def streamed(q, x):
        cx, cy, cz = lattice_moves[q]
        sx = x - cx
        inside = 0 <= sx < lx
        sx_wrapped = sx % lx
        v = pop[q, sx] if inside else land_x[side(cx) * faces // 2 + place_in(q, 0)]
        if cy and split_y:
            at = ly - 1 if cy > 0 else 0
            if inside:
                other = face_y[side(cy), place_in(q, 1), sx:sx + 1, :]
            else:
                other = edge_xy[edges_xy.index(q), sx_wrapped:sx_wrapped + 1, :]
            v = jnp.where(row == at, jnp.broadcast_to(other, v.shape), v)
        if cz:
            at = lz - 1 if cz > 0 else 0
            if inside:
                other = face_z[side(cz)]
                if cy and split_y:
                    at_y = ly - 1 if cy > 0 else 0
                    other = jnp.where(row == at_y, edge_yz[edges_yz.index(q)], other)
                k = place_in(q, 2) * lx + sx
                other = rolled(other, at - k, 1)
            else:
                other = land_x[edge_slot[cx, cz % nz]]
            v = jnp.where(lane == at, other, v)
        if cy:
            v = rolled(v, cy, 0)
        if cz:
            v = rolled(v, cz, 1)
        return v

    def advance(x):
        result = collided([streamed(q, x) for q in range(count_q)])
        for q in range(count_q):
            out_vm[q, x] = result[q]

    def group_up(group, carry):
        first = jnp.maximum(group * span, me + 1)
        last = jnp.minimum(group * span + span, nx)
        count = jnp.maximum(last - first, 0)
        for at, above in higher_around:
            count = count + jnp.where(at == group, above, 0)
        wait_some(ack_sem.at[1 + group], count)
        send_faces(lambda offset: (rank_of(offset) > rank) & (device_at(offset)[0] // span == group))
        lax.fori_loop(first, last, send_each, 0)
        return carry

    def go_up():
        lax.fori_loop(me // span, ack_groups, group_up, 0)

    if split_y:
        go_up()
        for sign in (1, -1):
            at = ly - 1 if sign > 0 else 0
            for i, q in enumerate(movers(1, sign)):
                for x in range(lx):
                    row_y[side(sign), i, x:x + 1, :] = pop[q, x, at:at + 1, :]
        for sign in (1, -1):
            s = side(sign)
            send_y(row_y.at[s], face_y.at[s], (0, sign, 0))
        for i, q in enumerate(edges_yz):
            s = side(lattice_moves[q][2])
            send_y(pack_z.at[s], edge_yz.at[i], lattice_moves[q])
        for i, q in enumerate(edges_xy):
            s = side(lattice_moves[q][1])
            send_y(row_y.at[s, place_in(q, 1)], edge_xy.at[i], lattice_moves[q])
    all_z.wait_recv()
    for copy in y_copies:
        copy.wait_recv()
    for x in range(1, lx - 1):
        advance(x)
    if not split_y:
        go_up()
    all_x.wait_recv()
    advance(0)
    advance(lx - 1)

    for copy in [all_x, all_z, all_m] + y_copies:
        copy.wait_send()
    all_m.wait_recv()


def finish(next_vm, recv_m, next_ref, slab_ref, slab_vm, sems):
    store = pltpu.make_async_copy(next_vm, next_ref, sems.at[0])
    store.start()
    _, lx, ly, lz = slab_vm.shape
    for p in range(2):
        square = recv_m[:, p].reshape(lz, lz).T
        slab_vm[2 * p:2 * p + 2] = square.reshape(2, lx, ly, lz)
    slab_store = pltpu.make_async_copy(slab_vm, slab_ref, sems.at[1])
    slab_store.start()
    store.wait()
    slab_store.wait()


def on_device(axes, sizes, populations):
    q, lx, ly, lz = populations.shape
    nx, ny, nz = (sizes[a] for a in axes)
    faces = 2 * len(movers(0, 1))
    edges = 4 if nz > 2 else 2
    f32 = jnp.float32
    tile = (ly, lz)
    y_sems = [pltpu.SemaphoreType.DMA((10,))] * 2 if ny > 1 else []
    held = pl.pallas_call(
        functools.partial(kernel, axes, sizes),
        out_shape=(
            pltpu.VMEM(populations.shape, f32),
            pltpu.VMEM((nx, 2, lx, lz), f32),
        ),
        in_specs=[pl.BlockSpec(memory_space=pl.ANY)],
        out_specs=(pl.BlockSpec(memory_space=pltpu.VMEM),) * 2,
        scratch_shapes=[
            pltpu.VMEM(populations.shape, f32),
            pltpu.VMEM((faces + edges,) + tile, f32),
            pltpu.VMEM((2,) + tile, f32),
            pltpu.VMEM((2,) + tile, f32),
            pltpu.VMEM((2,) + tile, f32),
            pltpu.VMEM((nx, 2, lx, lz), f32),
            pltpu.VMEM((2, 5, lx, lz), f32),
            pltpu.VMEM((2, 5, lx, lz), f32),
            pltpu.VMEM((4, lx, lz), f32),
            pltpu.VMEM((4,) + tile, f32),
            pltpu.SemaphoreType.DMA((len(load_chunks),)),
            pltpu.SemaphoreType.DMA((3,)),
            pltpu.SemaphoreType.DMA((3,)),
            pltpu.SemaphoreType.REGULAR((1 + ack_groups,)),
        ] + y_sems,
        compiler_params=pltpu.CompilerParams(collective_id=0, has_side_effects=True),
        name="lattice_step",
    )(populations)
    held = [pltpu.with_memory_space_constraint(h, pltpu.VMEM) for h in held]
    slab = (4, lx, ly, lz)
    return pl.pallas_call(
        finish,
        out_shape=(jax.ShapeDtypeStruct(populations.shape, f32), jax.ShapeDtypeStruct(slab, f32)),
        in_specs=[pl.BlockSpec(memory_space=pltpu.VMEM)] * 2,
        out_specs=(pl.BlockSpec(memory_space=pl.ANY),) * 2,
        scratch_shapes=[pltpu.VMEM(slab, f32), pltpu.SemaphoreType.DMA((2,))],
        name="finish",
    )(*held)


def solution(mesh):
    axes = tuple(mesh.axis_names)
    sizes = dict(mesh.shape)
    return jax.shard_map(
        functools.partial(on_device, axes, sizes),
        mesh=mesh,
        in_specs=(P(None, "gx", "gy", "gz"),),
        out_specs=(P(None, "gx", "gy", "gz"), P(None, ("gz", "gx"), "gy", None)),
        check_vma=False,
    )
```

```python
import functools

import jax
import jax.numpy as jnp
from jax import lax
from jax.experimental import pallas as pl
from jax.experimental.pallas import tpu as pltpu
from jax.sharding import PartitionSpec as P

MESH = pl.DeviceIdType.MESH

lattice_moves = [
    (0, 0, 0),
    (1, 0, 0),
    (-1, 0, 0),
    (0, 1, 0),
    (0, -1, 0),
    (0, 0, 1),
    (0, 0, -1),
    (1, 1, 0),
    (-1, -1, 0),
    (1, -1, 0),
    (-1, 1, 0),
    (1, 0, 1),
    (-1, 0, -1),
    (1, 0, -1),
    (-1, 0, 1),
    (0, 1, 1),
    (0, -1, -1),
    (0, 1, -1),
    (0, -1, 1),
]
lattice_weights = [1.0 / 3.0] + [1.0 / 18.0] * 6 + [1.0 / 36.0] * 12
relaxation = 1.6
count_q = len(lattice_moves)


def movers(component, sign):
    return [q for q, move in enumerate(lattice_moves) if move[component] == sign]


def place_in(q, component):
    return movers(component, lattice_moves[q][component]).index(q)


def side(sign):
    return 0 if sign > 0 else 1


edges_xz = [q for q, m in enumerate(lattice_moves) if m[0] and m[2]]
edges_xy = [q for q, m in enumerate(lattice_moves) if m[0] and m[1]]
edges_yz = [q for q, m in enumerate(lattice_moves) if m[1] and m[2]]


def total(terms):
    terms = list(terms)
    while len(terms) > 1:
        terms = [
            terms[i] + terms[i + 1] if i + 1 < len(terms) else terms[i]
            for i in range(0, len(terms), 2)
        ]
    return terms[0]


def moments_of(f):
    density = total(f)
    inverse = 1.0 / density
    velocity = []
    for component in range(3):
        plus = total(f[q] for q in movers(component, 1))
        minus = total(f[q] for q in movers(component, -1))
        velocity.append((plus - minus) * inverse)
    return density, velocity


def collided(f):
    density, velocity = moments_of(f)
    speed_sq = velocity[0] * velocity[0] + velocity[1] * velocity[1] + velocity[2] * velocity[2]
    base = 1.0 - 1.5 * speed_sq
    scaled = {w: (relaxation * w) * density for w in set(lattice_weights)}
    keep = 1.0 - relaxation
    result = [None] * count_q
    result[0] = keep * f[0] + scaled[lattice_weights[0]] * base
    for q in range(1, count_q, 2):
        move = lattice_moves[q]
        projected = None
        for component in range(3):
            if move[component] == 0:
                continue
            if projected is None:
                projected = velocity[component] if move[component] > 0 else -velocity[component]
            elif move[component] > 0:
                projected = projected + velocity[component]
            else:
                projected = projected - velocity[component]
        even = base + 4.5 * (projected * projected)
        odd = 3.0 * projected
        weight = scaled[lattice_weights[q]]
        result[q] = keep * f[q] + weight * (even + odd)
        result[q + 1] = keep * f[q + 1] + weight * (even - odd)
    return result


def rolled(v, shift, axis):
    return pltpu.roll(v, shift % v.shape[axis], axis)


def digits(at):
    return at % 2, at // 2 % 2, at // 4


def meets(low, high, nx):
    near = high - low in (1, nx - 1)
    below = all(a <= b for a, b in zip(digits(low), digits(high)))
    return low < high and (near or below or high == nx - 1)


def load_chunks(lx):
    return ((lx // 2, lx), (0, lx // 2))


def kernel(axes, sizes, pop_hbm, out_vm, recv_m,
           pop, land_x, face_z, pack_x, pack_z, send_m,
           row_y, face_y, edge_xy, edge_yz):
    nx, ny, nz = (sizes[a] for a in axes)
    here = tuple(lax.axis_index(a) for a in axes)
    me = here[0]
    _, lx, ly, lz = pop.shape
    split_y = ny > 1
    faces = len(movers(0, 1))
    last = nx - 1
    rank = (me * ny + here[1]) * nz + here[2]
    order = sorted(range(nx), key=lambda at: (sum(digits(at)), at))

    def device_at(offset):
        return tuple(
            lax.rem(h + o % n, n) if o % n else h
            for h, o, n in zip(here, offset, (nx, ny, nz))
        )

    def rank_of(offset):
        a, b, c = device_at(offset)
        return (a * ny + b) * nz + c

    def column(target):
        return (target,) + here[1:]

    def lookup(values):
        value = jnp.int32(values[0])
        for at in range(1, nx):
            value = jnp.where(me == at, values[at], value)
        return value

    def mask(chosen):
        return lookup([sum(1 << t for t in range(nx) if chosen(at, t)) for at in range(nx)])

    offsets = [(0, 0, 1), (0, 0, -1)]
    offsets += [lattice_moves[q] for q in edges_xz]
    if split_y:
        offsets += [(0, 1, 0), (0, -1, 0)]
        offsets += [lattice_moves[q] for q in edges_xy + edges_yz]
    around = sorted({(a % nx, b % ny, c % nz) for a, b, c in offsets})

    def scoped(load_sem, send_sem, recv_sem, ack_sem, around_sem, *y_sems):
        loads = []
        for i, (first, end) in enumerate(load_chunks(lx)):
            planes = pl.ds(first, end - first)
            load = pltpu.make_async_copy(pop_hbm.at[:, planes], pop.at[:, planes], load_sem.at[i])
            load.start()
            loads.append(load)

        up = mask(lambda at, t: meets(at, t, nx))
        down = mask(lambda at, t: meets(t, at, nx))
        aside = mask(lambda at, t: at != t and not meets(at, t, nx) and not meets(t, at, nx))

        def each(chosen, targets):
            def run(body):
                for at in targets:
                    pl.when((chosen & (1 << at)) != 0)(functools.partial(body, at))
            return run

        barrier = pltpu.get_barrier_semaphore()
        lower = lookup([sum(meets(t, at, nx) for t in range(nx)) for at in range(nx)])

        @each(up, order)
        def _(at):
            pl.semaphore_signal(barrier, inc=1, device_id=column(at), device_id_type=MESH)

        for offset in around:
            @pl.when(rank_of(offset) > rank)
            def _():
                pl.semaphore_signal(barrier, inc=1, device_id=device_at(offset), device_id_type=MESH)

            lower = lower + jnp.where(rank_of(offset) < rank, 1, 0)

        @pl.when(lower > 0)
        def _():
            pl.semaphore_wait(barrier, lower)

        for offset in around:
            back = tuple(-o % n for o, n in zip(offset, (nx, ny, nz)))

            @pl.when(rank_of(offset) < rank)
            def _():
                pl.semaphore_signal(
                    around_sem.at[around.index(back)], inc=1,
                    device_id=device_at(offset), device_id_type=MESH)

        @each(down, order)
        def _(at):
            pl.semaphore_signal(ack_sem.at[me], inc=1, device_id=column(at), device_id_type=MESH)

        lane = lax.broadcasted_iota(jnp.int32, (ly, lz), 1)
        row = lax.broadcasted_iota(jnp.int32, (ly, lz), 0)

        def remote(src, dst, kind, slot, offset):
            return pltpu.make_async_remote_copy(
                src_ref=src, dst_ref=dst, send_sem=send_sem.at[kind], recv_sem=recv_sem.at[slot],
                device_id=device_at(offset), device_id_type=MESH)

        y_copies = []

        def send_y(src, dst, offset):
            i = len(y_copies)
            copy = pltpu.make_async_remote_copy(
                src_ref=src, dst_ref=dst, send_sem=y_sems[0].at[i], recv_sem=y_sems[1].at[i],
                device_id=device_at(offset), device_id_type=MESH)
            copy.start()
            y_copies.append(copy)

        edge_steps = []
        for cz in (1, -1):
            if cz % nz not in edge_steps:
                edge_steps.append(cz % nz)

        def pack_edge(sign):
            at = lx - 1 if sign > 0 else 0
            forth, back = (lattice_moves.index((sign, 0, cz)) for cz in (1, -1))
            pack_x[side(sign)] = jnp.where(lane == lz - 1, pop[forth, at], pop[back, at])

        def send_face(sign):
            s, at = side(sign), lx - 1 if sign > 0 else 0
            for j, q in enumerate(movers(0, sign)):
                remote(pop.at[q, at], land_x.at[s, j], s, s, (sign, 0, 0)).start()
            for j, cz in enumerate(edge_steps):
                remote(pack_x.at[s], land_x.at[s, faces + j], s, s, (sign, 0, cz)).start()

        def send_moments(target):
            pltpu.make_async_remote_copy(
                src_ref=send_m.at[target], dst_ref=recv_m.at[me],
                send_sem=send_sem.at[3], recv_sem=recv_sem.at[3],
                device_id=column(target), device_id_type=MESH).start()

        def send_z(sign):
            remote(pack_z.at[side(sign)], face_z.at[side(sign)], 2, 2, (0, 0, sign)).start()

        lane_x = lane & (lx - 1)
        turned = [[None] * lx for _ in range(4)]

        def measure(x):
            density, velocity = moments_of([pop[q, x] for q in range(count_q)])
            for c, value in enumerate([density] + velocity):
                for z in range(lx):
                    moved = rolled(value, x - z, 1) if x != z else value
                    held = turned[c][z]
                    turned[c][z] = moved if held is None else jnp.where(lane_x == x, moved, held)

        for i, (first, end) in enumerate(load_chunks(lx)):
            loads[i].wait()
            if first <= lx - 1 < end:
                pack_edge(1)

                @pl.when(rank_of((1, 0, 0)) < rank)
                def _():
                    send_face(1)

            for x in range(first, end):
                measure(x)

        for p in range(2):
            square = jnp.concatenate(turned[2 * p] + turned[2 * p + 1], axis=0).T
            for j in range(nx):
                send_m[j, p] = square[j * lx:(j + 1) * lx]

        each(down, order)(send_moments)

        pack_edge(-1)

        @pl.when(rank_of((-1, 0, 0)) < rank)
        def _():
            send_face(-1)

        for sign in (1, -1):
            at = lz - 1 if sign > 0 else 0
            packed = jnp.zeros((ly, lz), jnp.float32)
            for i, q in enumerate(movers(2, sign)):
                for x in range(lx):
                    k = i * lx + x
                    packed = jnp.where(lane == k, rolled(pop[q, x], k - at, 1), packed)
            pack_z[side(sign)] = packed
        for offset in around:
            if offset[0] == offset[1] == 0:
                @pl.when(rank_of(offset) > rank)
                def _():
                    pl.semaphore_wait(around_sem.at[around.index(offset)], 1)
        for sign in (1, -1):
            send_z(sign)
        recv_m[me] = send_m[me]

        all_x = [remote(land_x.at[s], land_x.at[s], s, s, (1, 0, 0)) for s in range(2)]
        all_z = remote(face_z, face_z, 2, 2, (0, 0, 1))
        others = pl.ds(0, nx - 1)
        all_m = remote(send_m.at[others], send_m.at[others], 3, 3, (1, 0, 0))

        def streamed(q, x):
            cx, cy, cz = lattice_moves[q]
            sx = x - cx
            inside = 0 <= sx < lx
            sx_wrapped = sx % lx
            v = pop[q, sx] if inside else land_x[side(cx), place_in(q, 0)]
            if cy and split_y:
                at = ly - 1 if cy > 0 else 0
                if inside:
                    other = face_y[side(cy), place_in(q, 1), sx:sx + 1, :]
                else:
                    other = edge_xy[edges_xy.index(q), sx_wrapped:sx_wrapped + 1, :]
                v = jnp.where(row == at, jnp.broadcast_to(other, v.shape), v)
            if cz:
                at = lz - 1 if cz > 0 else 0
                if inside:
                    other = face_z[side(cz)]
                    if cy and split_y:
                        at_y = ly - 1 if cy > 0 else 0
                        other = jnp.where(row == at_y, edge_yz[edges_yz.index(q)], other)
                    k = place_in(q, 2) * lx + sx
                    other = rolled(other, at - k, 1)
                else:
                    other = land_x[side(cx), faces + edge_steps.index(cz % nz)]
                v = jnp.where(lane == at, other, v)
            if cy:
                v = rolled(v, cy, 0)
            if cz:
                v = rolled(v, cz, 1)
            return v

        def advance(x):
            result = collided([streamed(q, x) for q in range(count_q)])
            for q in range(count_q):
                out_vm[q, x] = result[q]

        def go_up():
            @each(up, order)
            def _(at):
                pl.semaphore_wait(ack_sem.at[at], 1)
                if at != last:
                    send_moments(at)

            for offset in around:
                if offset[0] or offset[1]:
                    @pl.when(rank_of(offset) > rank)
                    def _():
                        pl.semaphore_wait(around_sem.at[around.index(offset)], 1)

            for sign in (-1, 1):
                @pl.when(rank_of((sign, 0, 0)) > rank)
                def _():
                    send_face(sign)

            @pl.when(me != last)
            def _():
                send_moments(last)

            each(aside, order)(send_moments)

        if split_y:
            go_up()
            for sign in (1, -1):
                at = ly - 1 if sign > 0 else 0
                for i, q in enumerate(movers(1, sign)):
                    for x in range(lx):
                        row_y[side(sign), i, x:x + 1, :] = pop[q, x, at:at + 1, :]
            for sign in (1, -1):
                send_y(row_y.at[side(sign)], face_y.at[side(sign)], (0, sign, 0))
            for i, q in enumerate(edges_yz):
                send_y(pack_z.at[side(lattice_moves[q][2])], edge_yz.at[i], lattice_moves[q])
            for i, q in enumerate(edges_xy):
                send_y(row_y.at[side(lattice_moves[q][1]), place_in(q, 1)], edge_xy.at[i], lattice_moves[q])

        all_z.wait_recv()
        for copy in y_copies:
            copy.wait_recv()
        for x in range(1, lx - 1):
            advance(x)
        if not split_y:
            go_up()
        all_x[1].wait_recv()
        advance(lx - 1)
        all_x[0].wait_recv()
        advance(0)

        for copy in all_x + [all_z, all_m] + y_copies:
            copy.wait_send()
        all_m.wait_recv()

    dma = pltpu.SemaphoreType.DMA
    y_sems = [dma((10,))] * 2 if split_y else []
    pl.run_scoped(
        scoped, dma((len(load_chunks(lx)),)), dma((4,)), dma((4,)),
        pltpu.SemaphoreType.REGULAR((nx,)), pltpu.SemaphoreType.REGULAR((len(around),)), *y_sems)


def finish(next_vm, recv_m, next_ref, slab_ref, slab_vm):
    def scoped(sems):
        store = pltpu.make_async_copy(next_vm, next_ref, sems.at[0])
        store.start()
        _, lx, ly, lz = slab_vm.shape
        for p in range(2):
            square = recv_m[:, p].reshape(lz, lz).T
            slab_vm[2 * p:2 * p + 2] = square.reshape(2, lx, ly, lz)
        slab_store = pltpu.make_async_copy(slab_vm, slab_ref, sems.at[1])
        slab_store.start()
        store.wait()
        slab_store.wait()

    pl.run_scoped(scoped, pltpu.SemaphoreType.DMA((2,)))


def on_device(axes, sizes, populations):
    q, lx, ly, lz = populations.shape
    nx, ny, nz = (sizes[a] for a in axes)
    faces = len(movers(0, 1))
    edges = 2 if nz > 2 else 1
    f32 = jnp.float32
    tile = (ly, lz)
    held = pl.pallas_call(
        functools.partial(kernel, axes, sizes),
        out_shape=(
            pltpu.VMEM(populations.shape, f32),
            pltpu.VMEM((nx, 2, lx, lz), f32),
        ),
        in_specs=[pl.BlockSpec(memory_space=pl.ANY)],
        out_specs=(pl.BlockSpec(memory_space=pltpu.VMEM),) * 2,
        scratch_shapes=[
            pltpu.VMEM(populations.shape, f32),
            pltpu.VMEM((2, faces + edges) + tile, f32),
            pltpu.VMEM((2,) + tile, f32),
            pltpu.VMEM((2,) + tile, f32),
            pltpu.VMEM((2,) + tile, f32),
            pltpu.VMEM((nx, 2, lx, lz), f32),
            pltpu.VMEM((2, 5, lx, lz), f32),
            pltpu.VMEM((2, 5, lx, lz), f32),
            pltpu.VMEM((4, lx, lz), f32),
            pltpu.VMEM((4,) + tile, f32),
        ],
        compiler_params=pltpu.CompilerParams(collective_id=0, has_side_effects=True),
        name="lattice_step",
    )(populations)
    held = [pltpu.with_memory_space_constraint(h, pltpu.VMEM) for h in held]
    slab = (4, lx, ly, lz)
    return pl.pallas_call(
        finish,
        out_shape=(jax.ShapeDtypeStruct(populations.shape, f32), jax.ShapeDtypeStruct(slab, f32)),
        in_specs=[pl.BlockSpec(memory_space=pltpu.VMEM)] * 2,
        out_specs=(pl.BlockSpec(memory_space=pl.ANY),) * 2,
        scratch_shapes=[pltpu.VMEM(slab, f32)],
        name="finish",
    )(*held)


def solution(mesh):
    axes = tuple(mesh.axis_names)
    sizes = dict(mesh.shape)
    return jax.shard_map(
        functools.partial(on_device, axes, sizes),
        mesh=mesh,
        in_specs=(P(None, "gx", "gy", "gz"),),
        out_specs=(P(None, "gx", "gy", "gz"), P(None, ("gz", "gx"), "gy", None)),
        check_vma=False,
    )
```

```python
import functools

import jax
import jax.numpy as jnp
from jax import lax
from jax.experimental import pallas as pl
from jax.experimental.pallas import tpu as pltpu
from jax.sharding import PartitionSpec as P

MESH = pl.DeviceIdType.MESH

lattice_moves = [
    (0, 0, 0),
    (1, 0, 0),
    (-1, 0, 0),
    (0, 1, 0),
    (0, -1, 0),
    (0, 0, 1),
    (0, 0, -1),
    (1, 1, 0),
    (-1, -1, 0),
    (1, -1, 0),
    (-1, 1, 0),
    (1, 0, 1),
    (-1, 0, -1),
    (1, 0, -1),
    (-1, 0, 1),
    (0, 1, 1),
    (0, -1, -1),
    (0, 1, -1),
    (0, -1, 1),
]
lattice_weights = [1.0 / 3.0] + [1.0 / 18.0] * 6 + [1.0 / 36.0] * 12
relaxation = 1.6
count_q = len(lattice_moves)


def movers(component, sign):
    return [q for q, move in enumerate(lattice_moves) if move[component] == sign]


def place_in(q, component):
    return movers(component, lattice_moves[q][component]).index(q)


def side(sign):
    return 0 if sign > 0 else 1


edges_xz = [q for q, m in enumerate(lattice_moves) if m[0] and m[2]]
edges_xy = [q for q, m in enumerate(lattice_moves) if m[0] and m[1]]
edges_yz = [q for q, m in enumerate(lattice_moves) if m[1] and m[2]]


def total(terms):
    terms = list(terms)
    while len(terms) > 1:
        terms = [
            terms[i] + terms[i + 1] if i + 1 < len(terms) else terms[i]
            for i in range(0, len(terms), 2)
        ]
    return terms[0]


def moments_of(f):
    density = total(f)
    inverse = 1.0 / density
    velocity = []
    for component in range(3):
        plus = total(f[q] for q in movers(component, 1))
        minus = total(f[q] for q in movers(component, -1))
        velocity.append((plus - minus) * inverse)
    return density, velocity


def collided(f):
    density, velocity = moments_of(f)
    speed_sq = velocity[0] * velocity[0] + velocity[1] * velocity[1] + velocity[2] * velocity[2]
    base = 1.0 - 1.5 * speed_sq
    scaled = {w: (relaxation * w) * density for w in set(lattice_weights)}
    keep = 1.0 - relaxation
    result = [None] * count_q
    result[0] = keep * f[0] + scaled[lattice_weights[0]] * base
    for q in range(1, count_q, 2):
        move = lattice_moves[q]
        projected = None
        for component in range(3):
            if move[component] == 0:
                continue
            if projected is None:
                projected = velocity[component] if move[component] > 0 else -velocity[component]
            elif move[component] > 0:
                projected = projected + velocity[component]
            else:
                projected = projected - velocity[component]
        even = base + 4.5 * (projected * projected)
        odd = 3.0 * projected
        weight = scaled[lattice_weights[q]]
        result[q] = keep * f[q] + weight * (even + odd)
        result[q + 1] = keep * f[q + 1] + weight * (even - odd)
    return result


def rolled(v, shift, axis):
    return pltpu.roll(v, shift % v.shape[axis], axis)


def digits(at):
    return at % 2, at // 2 % 2, at // 4


def entry_order(nx):
    return sorted(range(nx), key=lambda at: (sum(digits(at)), at))


def meets(low, high, nx):
    below = all(a <= b for a, b in zip(digits(low), digits(high)))
    return low != high and (below or high == entry_order(nx)[-1]) and low != entry_order(nx)[-1]


def load_chunks(lx):
    return ((lx - 2, lx), (0, lx - 2))


def kernel(axes, sizes, pop_hbm, out_vm, recv_m,
           pop, land_x, face_z, pack_x, pack_z, send_m,
           row_y, face_y, edge_xy, edge_yz):
    nx, ny, nz = (sizes[a] for a in axes)
    here = tuple(lax.axis_index(a) for a in axes)
    me = here[0]
    _, lx, ly, lz = pop.shape
    split_y = ny > 1
    faces = len(movers(0, 1))
    order = entry_order(nx)
    last = order[-1]

    def device_at(offset):
        return tuple(
            lax.rem(h + o % n, n) if o % n else h
            for h, o, n in zip(here, offset, (nx, ny, nz))
        )

    def column(target):
        return (target,) + here[1:]

    def lookup(values):
        value = jnp.int32(values[0])
        for at in range(1, nx):
            value = jnp.where(me == at, values[at], value)
        return value

    def step_bits(relation):
        return lookup([
            relation(at, (at + 1) % nx) + 2 * relation(at, (at - 1) % nx) for at in range(nx)])

    beside_lower = step_bits(lambda at, t: int(meets(t, at, nx)))
    beside_higher = step_bits(lambda at, t: int(meets(at, t, nx) and t != last))

    def beside(bits, offset):
        return (bits & (1 if offset[0] % nx == 1 else 2)) != 0

    def is_lower(offset):
        if offset[0]:
            return beside(beside_lower, offset)
        _, b, c = device_at(offset)
        return b * nz + c < here[1] * nz + here[2]

    def mask(chosen):
        return lookup([sum(1 << t for t in range(nx) if chosen(at, t)) for at in range(nx)])

    offsets = [(0, 0, 1), (0, 0, -1)]
    offsets += [lattice_moves[q] for q in edges_xz]
    if split_y:
        offsets += [(0, 1, 0), (0, -1, 0)]
        offsets += [lattice_moves[q] for q in edges_xy + edges_yz]
    around = sorted({(a % nx, b % ny, c % nz) for a, b, c in offsets})

    adjacent = sorted({o[1:] for o in around if o[0]})

    def scoped(load_sem, send_sem, recv_sem, ack_sem, around_sem, *y_sems):
        loads = []
        for i, (first, end) in enumerate(load_chunks(lx)):
            planes = pl.ds(first, end - first)
            load = pltpu.make_async_copy(pop_hbm.at[:, planes], pop.at[:, planes], load_sem.at[i])
            load.start()
            loads.append(load)

        up = mask(lambda at, t: meets(at, t, nx))
        down = mask(lambda at, t: meets(t, at, nx))
        aside = mask(lambda at, t: at != t and not meets(at, t, nx) and not meets(t, at, nx))

        def each(chosen, targets):
            def run(body):
                for at in targets:
                    pl.when((chosen & (1 << at)) != 0)(functools.partial(body, at))
            return run

        barrier = pltpu.get_barrier_semaphore()
        lower = lookup([sum(meets(t, at, nx) for t in range(nx)) for at in range(nx)])

        @each(up, order)
        def _(at):
            pl.semaphore_signal(barrier, inc=1, device_id=column(at), device_id_type=MESH)

        for offset in around:
            goes = beside(beside_higher, offset) if offset[0] else jnp.logical_not(is_lower(offset))

            @pl.when(goes)
            def _():
                pl.semaphore_signal(barrier, inc=1, device_id=device_at(offset), device_id_type=MESH)

            comes = jnp.logical_and(is_lower(offset), me != last) if offset[0] else is_lower(offset)
            lower = lower + jnp.where(comes, 1, 0)
        for b, c in adjacent:
            _, there_b, there_c = device_at((0, b, c))

            @pl.when(me != last)
            def _():
                pl.semaphore_signal(
                    barrier, inc=1, device_id=(last, there_b, there_c), device_id_type=MESH)

        lower = lower + jnp.where(me == last, len(adjacent) * (nx - 1), 0)

        @pl.when(lower > 0)
        def _():
            pl.semaphore_wait(barrier, lower)

        for offset in around:
            back = tuple(-o % n for o, n in zip(offset, (nx, ny, nz)))

            @pl.when(me == last if offset[0] else is_lower(offset))
            def _():
                pl.semaphore_signal(
                    around_sem.at[around.index(back)], inc=1,
                    device_id=device_at(offset), device_id_type=MESH)

        @each(down, order)
        def _(at):
            pl.semaphore_signal(ack_sem.at[me], inc=1, device_id=column(at), device_id_type=MESH)

        lane = lax.broadcasted_iota(jnp.int32, (ly, lz), 1)
        row = lax.broadcasted_iota(jnp.int32, (ly, lz), 0)

        def remote(src, dst, kind, slot, offset):
            return pltpu.make_async_remote_copy(
                src_ref=src, dst_ref=dst, send_sem=send_sem.at[kind], recv_sem=recv_sem.at[slot],
                device_id=device_at(offset), device_id_type=MESH)

        y_copies = []

        def send_y(src, dst, offset):
            i = len(y_copies)
            copy = pltpu.make_async_remote_copy(
                src_ref=src, dst_ref=dst, send_sem=y_sems[0].at[i], recv_sem=y_sems[1].at[i],
                device_id=device_at(offset), device_id_type=MESH)
            copy.start()
            y_copies.append(copy)

        edge_steps = []
        for cz in (1, -1):
            if cz % nz not in edge_steps:
                edge_steps.append(cz % nz)

        def pack_edge(sign):
            at = lx - 1 if sign > 0 else 0
            forth, back = (lattice_moves.index((sign, 0, cz)) for cz in (1, -1))
            pack_x[side(sign)] = jnp.where(lane == lz - 1, pop[forth, at], pop[back, at])

        def send_face(sign):
            s, at = side(sign), lx - 1 if sign > 0 else 0
            for j, q in enumerate(movers(0, sign)):
                remote(pop.at[q, at], land_x.at[s, j], s, s, (sign, 0, 0)).start()
            for j, cz in enumerate(edge_steps):
                remote(pack_x.at[s], land_x.at[s, faces + j], s, s, (sign, 0, cz)).start()

        def send_moments(target):
            pltpu.make_async_remote_copy(
                src_ref=send_m.at[target], dst_ref=recv_m.at[me],
                send_sem=send_sem.at[3], recv_sem=recv_sem.at[3],
                device_id=column(target), device_id_type=MESH).start()

        def send_z(sign):
            remote(pack_z.at[side(sign)], face_z.at[side(sign)], 2, 2, (0, 0, sign)).start()

        lane_x = lane & (lx - 1)
        turned = [[None] * lx for _ in range(4)]

        def measure(x):
            density, velocity = moments_of([pop[q, x] for q in range(count_q)])
            for c, value in enumerate([density] + velocity):
                for z in range(lx):
                    moved = rolled(value, x - z, 1) if x != z else value
                    held = turned[c][z]
                    turned[c][z] = moved if held is None else jnp.where(lane_x == x, moved, held)

        for i, (first, end) in enumerate(load_chunks(lx)):
            loads[i].wait()
            if first <= lx - 1 < end:
                pack_edge(1)

                @pl.when(is_lower((1, 0, 0)))
                def _():
                    send_face(1)

            for x in range(first, end):
                measure(x)

        for p in range(2):
            square = jnp.concatenate(turned[2 * p] + turned[2 * p + 1], axis=0).T
            for j in range(nx):
                send_m[j, p] = square[j * lx:(j + 1) * lx]

        each(down, order[:5])(send_moments)

        pack_edge(-1)

        @pl.when(is_lower((-1, 0, 0)))
        def _():
            send_face(-1)

        for sign in (1, -1):
            at = lz - 1 if sign > 0 else 0
            packed = jnp.zeros((ly, lz), jnp.float32)
            for i, q in enumerate(movers(2, sign)):
                for x in range(lx):
                    k = i * lx + x
                    packed = jnp.where(lane == k, rolled(pop[q, x], k - at, 1), packed)
            pack_z[side(sign)] = packed
        for offset in around:
            if offset[0] == offset[1] == 0:
                @pl.when(jnp.logical_not(is_lower(offset)))
                def _():
                    pl.semaphore_wait(around_sem.at[around.index(offset)], 1)
        for sign in (1, -1):
            send_z(sign)
        each(down, order[5:])(send_moments)
        recv_m[me] = send_m[me]

        all_x = [remote(land_x.at[s], land_x.at[s], s, s, (1, 0, 0)) for s in range(2)]
        all_z = remote(face_z, face_z, 2, 2, (0, 0, 1))
        others = pl.ds(0, nx - 1)
        all_m = remote(send_m.at[others], send_m.at[others], 3, 3, (1, 0, 0))

        def streamed(q, x):
            cx, cy, cz = lattice_moves[q]
            sx = x - cx
            inside = 0 <= sx < lx
            sx_wrapped = sx % lx
            v = pop[q, sx] if inside else land_x[side(cx), place_in(q, 0)]
            if cy and split_y:
                at = ly - 1 if cy > 0 else 0
                if inside:
                    other = face_y[side(cy), place_in(q, 1), sx:sx + 1, :]
                else:
                    other = edge_xy[edges_xy.index(q), sx_wrapped:sx_wrapped + 1, :]
                v = jnp.where(row == at, jnp.broadcast_to(other, v.shape), v)
            if cz:
                at = lz - 1 if cz > 0 else 0
                if inside:
                    other = face_z[side(cz)]
                    if cy and split_y:
                        at_y = ly - 1 if cy > 0 else 0
                        other = jnp.where(row == at_y, edge_yz[edges_yz.index(q)], other)
                    k = place_in(q, 2) * lx + sx
                    other = rolled(other, at - k, 1)
                else:
                    other = land_x[side(cx), faces + edge_steps.index(cz % nz)]
                v = jnp.where(lane == at, other, v)
            if cy:
                v = rolled(v, cy, 0)
            if cz:
                v = rolled(v, cz, 1)
            return v

        def advance(x):
            result = collided([streamed(q, x) for q in range(count_q)])
            for q in range(count_q):
                out_vm[q, x] = result[q]

        def go_up():
            @each(up, order)
            def _(at):
                pl.semaphore_wait(ack_sem.at[at], 1)
                if at != last:
                    send_moments(at)

            for offset in around:
                if offset[0] or offset[1]:
                    @pl.when(me == (last - offset[0]) % nx if offset[0] else jnp.logical_not(is_lower(offset)))
                    def _():
                        pl.semaphore_wait(around_sem.at[around.index(offset)], 1)

            for sign in (-1, 1):
                @pl.when(jnp.logical_not(is_lower((sign, 0, 0))))
                def _():
                    send_face(sign)

            @pl.when(me != last)
            def _():
                send_moments(last)

            each(aside, order)(send_moments)

        go_up()
        if split_y:
            for sign in (1, -1):
                at = ly - 1 if sign > 0 else 0
                for i, q in enumerate(movers(1, sign)):
                    for x in range(lx):
                        row_y[side(sign), i, x:x + 1, :] = pop[q, x, at:at + 1, :]
            for sign in (1, -1):
                send_y(row_y.at[side(sign)], face_y.at[side(sign)], (0, sign, 0))
            for i, q in enumerate(edges_yz):
                send_y(pack_z.at[side(lattice_moves[q][2])], edge_yz.at[i], lattice_moves[q])
            for i, q in enumerate(edges_xy):
                send_y(row_y.at[side(lattice_moves[q][1]), place_in(q, 1)], edge_xy.at[i], lattice_moves[q])

        all_z.wait_recv()
        for copy in y_copies:
            copy.wait_recv()
        for x in range(1, lx - 1):
            advance(x)
        all_x[1].wait_recv()
        advance(lx - 1)
        all_x[0].wait_recv()
        advance(0)

        for copy in all_x + [all_z, all_m] + y_copies:
            copy.wait_send()
        all_m.wait_recv()

    dma = pltpu.SemaphoreType.DMA
    y_sems = [dma((10,))] * 2 if split_y else []
    pl.run_scoped(
        scoped, dma((len(load_chunks(lx)),)), dma((4,)), dma((4,)),
        pltpu.SemaphoreType.REGULAR((nx,)), pltpu.SemaphoreType.REGULAR((len(around),)), *y_sems)


def finish(next_vm, recv_m, next_ref, slab_ref, slab_vm):
    def scoped(sems):
        store = pltpu.make_async_copy(next_vm, next_ref, sems.at[0])
        store.start()
        _, lx, ly, lz = slab_vm.shape
        for p in range(2):
            square = recv_m[:, p].reshape(lz, lz).T
            slab_vm[2 * p:2 * p + 2] = square.reshape(2, lx, ly, lz)
        slab_store = pltpu.make_async_copy(slab_vm, slab_ref, sems.at[1])
        slab_store.start()
        store.wait()
        slab_store.wait()

    pl.run_scoped(scoped, pltpu.SemaphoreType.DMA((2,)))


def on_device(axes, sizes, populations):
    q, lx, ly, lz = populations.shape
    nx, ny, nz = (sizes[a] for a in axes)
    faces = len(movers(0, 1))
    edges = 2 if nz > 2 else 1
    f32 = jnp.float32
    tile = (ly, lz)
    held = pl.pallas_call(
        functools.partial(kernel, axes, sizes),
        out_shape=(
            pltpu.VMEM(populations.shape, f32),
            pltpu.VMEM((nx, 2, lx, lz), f32),
        ),
        in_specs=[pl.BlockSpec(memory_space=pl.ANY)],
        out_specs=(pl.BlockSpec(memory_space=pltpu.VMEM),) * 2,
        scratch_shapes=[
            pltpu.VMEM(populations.shape, f32),
            pltpu.VMEM((2, faces + edges) + tile, f32),
            pltpu.VMEM((2,) + tile, f32),
            pltpu.VMEM((2,) + tile, f32),
            pltpu.VMEM((2,) + tile, f32),
            pltpu.VMEM((nx, 2, lx, lz), f32),
            pltpu.VMEM((2, 5, lx, lz), f32),
            pltpu.VMEM((2, 5, lx, lz), f32),
            pltpu.VMEM((4, lx, lz), f32),
            pltpu.VMEM((4,) + tile, f32),
        ],
        compiler_params=pltpu.CompilerParams(collective_id=0, has_side_effects=True),
        name="lattice_step",
    )(populations)
    held = [pltpu.with_memory_space_constraint(h, pltpu.VMEM) for h in held]
    slab = (4, lx, ly, lz)
    return pl.pallas_call(
        finish,
        out_shape=(jax.ShapeDtypeStruct(populations.shape, f32), jax.ShapeDtypeStruct(slab, f32)),
        in_specs=[pl.BlockSpec(memory_space=pltpu.VMEM)] * 2,
        out_specs=(pl.BlockSpec(memory_space=pl.ANY),) * 2,
        scratch_shapes=[pltpu.VMEM(slab, f32)],
        name="finish",
    )(*held)


def solution(mesh):
    axes = tuple(mesh.axis_names)
    sizes = dict(mesh.shape)
    return jax.shard_map(
        functools.partial(on_device, axes, sizes),
        mesh=mesh,
        in_specs=(P(None, "gx", "gy", "gz"),),
        out_specs=(P(None, "gx", "gy", "gz"), P(None, ("gz", "gx"), "gy", None)),
        check_vma=False,
    )
```

```python
import functools

import jax
import jax.numpy as jnp
from jax import lax
from jax.experimental import pallas as pl
from jax.experimental.pallas import tpu as pltpu
from jax.sharding import PartitionSpec as P

MESH = pl.DeviceIdType.MESH

lattice_moves = [
    (0, 0, 0),
    (1, 0, 0),
    (-1, 0, 0),
    (0, 1, 0),
    (0, -1, 0),
    (0, 0, 1),
    (0, 0, -1),
    (1, 1, 0),
    (-1, -1, 0),
    (1, -1, 0),
    (-1, 1, 0),
    (1, 0, 1),
    (-1, 0, -1),
    (1, 0, -1),
    (-1, 0, 1),
    (0, 1, 1),
    (0, -1, -1),
    (0, 1, -1),
    (0, -1, 1),
]
lattice_weights = [1.0 / 3.0] + [1.0 / 18.0] * 6 + [1.0 / 36.0] * 12
relaxation = 1.6
count_q = len(lattice_moves)


def movers(component, sign):
    return [q for q, move in enumerate(lattice_moves) if move[component] == sign]


def place_in(q, component):
    return movers(component, lattice_moves[q][component]).index(q)


def side(sign):
    return 0 if sign > 0 else 1


edges_xz = [q for q, m in enumerate(lattice_moves) if m[0] and m[2]]
edges_xy = [q for q, m in enumerate(lattice_moves) if m[0] and m[1]]
edges_yz = [q for q, m in enumerate(lattice_moves) if m[1] and m[2]]


def total(terms):
    terms = list(terms)
    while len(terms) > 1:
        terms = [
            terms[i] + terms[i + 1] if i + 1 < len(terms) else terms[i]
            for i in range(0, len(terms), 2)
        ]
    return terms[0]


def moments_of(f):
    density = total(f)
    inverse = 1.0 / density
    velocity = []
    for component in range(3):
        plus = total(f[q] for q in movers(component, 1))
        minus = total(f[q] for q in movers(component, -1))
        velocity.append((plus - minus) * inverse)
    return density, velocity


def collided(f):
    density, velocity = moments_of(f)
    speed_sq = velocity[0] * velocity[0] + velocity[1] * velocity[1] + velocity[2] * velocity[2]
    base = 1.0 - 1.5 * speed_sq
    scaled = {w: (relaxation * w) * density for w in set(lattice_weights)}
    keep = 1.0 - relaxation
    result = [None] * count_q
    result[0] = keep * f[0] + scaled[lattice_weights[0]] * base
    for q in range(1, count_q, 2):
        move = lattice_moves[q]
        projected = None
        for component in range(3):
            if move[component] == 0:
                continue
            if projected is None:
                projected = velocity[component] if move[component] > 0 else -velocity[component]
            elif move[component] > 0:
                projected = projected + velocity[component]
            else:
                projected = projected - velocity[component]
        even = base + 4.5 * (projected * projected)
        odd = 3.0 * projected
        weight = scaled[lattice_weights[q]]
        result[q] = keep * f[q] + weight * (even + odd)
        result[q + 1] = keep * f[q + 1] + weight * (even - odd)
    return result


def rolled(v, shift, axis):
    return pltpu.roll(v, shift % v.shape[axis], axis)


def digits(at):
    return at % 2, at // 2 % 2, at // 4


def entry_order(nx):
    return sorted(range(nx), key=lambda at: (sum(digits(at)), at))


def meets(low, high, nx):
    below = all(a <= b for a, b in zip(digits(low), digits(high)))
    return low != high and (below or high == entry_order(nx)[-1]) and low != entry_order(nx)[-1]


def load_chunks(lx):
    return ((lx - 1, lx), (0, lx - 1))


def kernel(axes, sizes, pop_hbm, out_vm, recv_m,
           pop, land_x, face_z, turned, pack_x, pack_z, send_m,
           row_y, face_y, edge_xy, edge_yz):
    nx, ny, nz = (sizes[a] for a in axes)
    here = tuple(lax.axis_index(a) for a in axes)
    me = here[0]
    _, lx, ly, lz = pop.shape
    split_y = ny > 1
    faces = len(movers(0, 1))
    order = entry_order(nx)
    last = order[-1]

    def device_at(offset):
        return tuple(
            lax.rem(h + o % n, n) if o % n else h
            for h, o, n in zip(here, offset, (nx, ny, nz))
        )

    def column(target):
        return (target,) + here[1:]

    def lookup(values):
        value = jnp.int32(values[0])
        for at in range(1, nx):
            value = jnp.where(me == at, values[at], value)
        return value

    def step_bits(relation):
        return lookup([
            relation(at, (at + 1) % nx) + 2 * relation(at, (at - 1) % nx) for at in range(nx)])

    beside_lower = step_bits(lambda at, t: int(meets(t, at, nx)))
    beside_higher = step_bits(lambda at, t: int(meets(at, t, nx) and t != last))

    def beside(bits, offset):
        return (bits & (1 if offset[0] % nx == 1 else 2)) != 0

    def is_lower(offset):
        if offset[0]:
            return beside(beside_lower, offset)
        _, b, c = device_at(offset)
        return b * nz + c < here[1] * nz + here[2]

    def mask(chosen):
        return lookup([sum(1 << t for t in range(nx) if chosen(at, t)) for at in range(nx)])

    offsets = [(0, 0, 1), (0, 0, -1)]
    offsets += [lattice_moves[q] for q in edges_xz]
    if split_y:
        offsets += [(0, 1, 0), (0, -1, 0)]
        offsets += [lattice_moves[q] for q in edges_xy + edges_yz]
    around = sorted({(a % nx, b % ny, c % nz) for a, b, c in offsets})

    adjacent = sorted({o[1:] for o in around if o[0]})

    def scoped(load_sem, send_sem, recv_sem, ack_sem, around_sem, *y_sems):
        loads = []
        for i, (first, end) in enumerate(load_chunks(lx)):
            planes = pl.ds(first, end - first)
            load = pltpu.make_async_copy(pop_hbm.at[:, planes], pop.at[:, planes], load_sem.at[i])
            load.start()
            loads.append(load)

        up = mask(lambda at, t: meets(at, t, nx))
        down = mask(lambda at, t: meets(t, at, nx))
        aside = mask(lambda at, t: at != t and not meets(at, t, nx) and not meets(t, at, nx))

        def each(chosen, targets):
            def run(body):
                for at in targets:
                    pl.when((chosen & (1 << at)) != 0)(functools.partial(body, at))
            return run

        barrier = pltpu.get_barrier_semaphore()
        lower = lookup([sum(meets(t, at, nx) for t in range(nx)) for at in range(nx)])

        @each(up, order)
        def _(at):
            pl.semaphore_signal(barrier, inc=1, device_id=column(at), device_id_type=MESH)

        for offset in around:
            goes = beside(beside_higher, offset) if offset[0] else jnp.logical_not(is_lower(offset))

            @pl.when(goes)
            def _():
                pl.semaphore_signal(barrier, inc=1, device_id=device_at(offset), device_id_type=MESH)

            comes = jnp.logical_and(is_lower(offset), me != last) if offset[0] else is_lower(offset)
            lower = lower + jnp.where(comes, 1, 0)
        for b, c in adjacent:
            _, there_b, there_c = device_at((0, b, c))

            @pl.when(me != last)
            def _():
                pl.semaphore_signal(
                    barrier, inc=1, device_id=(last, there_b, there_c), device_id_type=MESH)

        lower = lower + jnp.where(me == last, len(adjacent) * (nx - 1), 0)

        @pl.when(lower > 0)
        def _():
            pl.semaphore_wait(barrier, lower)

        for offset in around:
            back = tuple(-o % n for o, n in zip(offset, (nx, ny, nz)))

            @pl.when(me == last if offset[0] else is_lower(offset))
            def _():
                pl.semaphore_signal(
                    around_sem.at[around.index(back)], inc=1,
                    device_id=device_at(offset), device_id_type=MESH)

        @each(down, order)
        def _(at):
            pl.semaphore_signal(ack_sem.at[me], inc=1, device_id=column(at), device_id_type=MESH)

        lane = lax.broadcasted_iota(jnp.int32, (ly, lz), 1)
        row = lax.broadcasted_iota(jnp.int32, (ly, lz), 0)

        def remote(src, dst, kind, slot, offset):
            return pltpu.make_async_remote_copy(
                src_ref=src, dst_ref=dst, send_sem=send_sem.at[kind], recv_sem=recv_sem.at[slot],
                device_id=device_at(offset), device_id_type=MESH)

        y_copies = []

        def send_y(src, dst, offset):
            i = len(y_copies)
            copy = pltpu.make_async_remote_copy(
                src_ref=src, dst_ref=dst, send_sem=y_sems[0].at[i], recv_sem=y_sems[1].at[i],
                device_id=device_at(offset), device_id_type=MESH)
            copy.start()
            y_copies.append(copy)

        edge_steps = []
        for cz in (1, -1):
            if cz % nz not in edge_steps:
                edge_steps.append(cz % nz)

        def pack_edge(sign):
            s, at = side(sign), lx - 1 if sign > 0 else 0
            for j, cz in enumerate((1, -1)):
                turned[s, j] = rolled(pop[lattice_moves.index((sign, 0, cz)), at], cz, 1)
            pack_x[s] = jnp.where(lane == 0, turned[s, 0], turned[s, 1])

        def send_plain(sign):
            s, at = side(sign), lx - 1 if sign > 0 else 0
            for j, q in enumerate(movers(0, sign)):
                if not lattice_moves[q][2]:
                    remote(pop.at[q, at], land_x.at[s, j], s, s, (sign, 0, 0)).start()

        def send_turned(sign):
            s = side(sign)
            for j, q in enumerate(movers(0, sign)):
                if lattice_moves[q][2]:
                    i = (1, -1).index(lattice_moves[q][2])
                    remote(turned.at[s, i], land_x.at[s, j], s, s, (sign, 0, 0)).start()
            for j, cz in enumerate(edge_steps):
                remote(pack_x.at[s], land_x.at[s, faces + j], s, s, (sign, 0, cz)).start()

        def send_face(sign):
            send_plain(sign)
            send_turned(sign)

        def send_moments(target):
            pltpu.make_async_remote_copy(
                src_ref=send_m.at[target], dst_ref=recv_m.at[me],
                send_sem=send_sem.at[3], recv_sem=recv_sem.at[3],
                device_id=column(target), device_id_type=MESH).start()

        def send_z(sign):
            remote(pack_z.at[side(sign)], face_z.at[side(sign)], 2, 2, (0, 0, sign)).start()

        lane_x = lane & (lx - 1)
        values = [[None] * lx for _ in range(4)]

        def measure(x):
            density, velocity = moments_of([pop[q, x] for q in range(count_q)])
            for c, value in enumerate([density] + velocity):
                values[c][x] = value

        def skewed(tiles):
            step = 1
            while step < lx:
                odd = (lane & step) != 0
                tiles = [jnp.where(odd, tiles[(k + step) % lx], tiles[k]) for k in range(lx)]
                step *= 2
            return tiles

        def exchanged(tiles):
            tiles = skewed(tiles)
            tiles = [tiles[0]] + [
                jnp.where(lane_x >= k, rolled(tiles[k], k, 1), rolled(tiles[k], k - lx, 1))
                for k in range(1, lx)]
            tiles = skewed(tiles)
            return [tiles[-z % lx] for z in range(lx)]

        for i, (first, end) in enumerate(load_chunks(lx)):
            loads[i].wait()
            if first <= lx - 1 < end:
                @pl.when(is_lower((1, 0, 0)))
                def _():
                    send_plain(1)

                pack_edge(1)

                @pl.when(is_lower((1, 0, 0)))
                def _():
                    send_turned(1)

            for x in range(first, end):
                measure(x)

        for p in range(2):
            rows = exchanged(values[2 * p]) + exchanged(values[2 * p + 1])
            square = jnp.concatenate(rows, axis=0).T
            for j in range(nx):
                send_m[j, p] = square[j * lx:(j + 1) * lx]

        early = jnp.where(here[2] == 0, down, 0)
        each(down, order[:1])(send_moments)
        each(early, order[1:1])(send_moments)

        pack_edge(-1)

        @pl.when(is_lower((-1, 0, 0)))
        def _():
            send_face(-1)

        for sign in (1, -1):
            at = lz - 1 if sign > 0 else 0
            packed = jnp.zeros((ly, lz), jnp.float32)
            for i, q in enumerate(movers(2, sign)):
                for x in range(lx):
                    k = i * lx + x
                    packed = jnp.where(lane == k, rolled(pop[q, x], k - at, 1), packed)
            pack_z[side(sign)] = packed
        for offset in around:
            if offset[0] == offset[1] == 0:
                @pl.when(jnp.logical_not(is_lower(offset)))
                def _():
                    pl.semaphore_wait(around_sem.at[around.index(offset)], 1)
        for sign in (1, -1):
            send_z(sign)
        each(early, order[1:])(send_moments)
        recv_m[me] = send_m[me]

        all_x = [remote(land_x.at[s], land_x.at[s], s, s, (1, 0, 0)) for s in range(2)]
        all_z = remote(face_z, face_z, 2, 2, (0, 0, 1))
        others = pl.ds(0, nx - 1)
        all_m = remote(send_m.at[others], send_m.at[others], 3, 3, (1, 0, 0))

        def streamed(q, x):
            cx, cy, cz = lattice_moves[q]
            sx = x - cx
            inside = 0 <= sx < lx
            sx_wrapped = sx % lx
            v = pop[q, sx] if inside else land_x[side(cx), place_in(q, 0)]
            if cy and split_y:
                at = ly - 1 if cy > 0 else 0
                if inside:
                    other = face_y[side(cy), place_in(q, 1), sx:sx + 1, :]
                else:
                    other = edge_xy[edges_xy.index(q), sx_wrapped:sx_wrapped + 1, :]
                v = jnp.where(row == at, jnp.broadcast_to(other, v.shape), v)
            if cz:
                at = lz - 1 if cz > 0 else 0
                if inside:
                    other = face_z[side(cz)]
                    if cy and split_y:
                        at_y = ly - 1 if cy > 0 else 0
                        other = jnp.where(row == at_y, edge_yz[edges_yz.index(q)], other)
                    k = place_in(q, 2) * lx + sx
                    other = rolled(other, at - k, 1)
                else:
                    other = land_x[side(cx), faces + edge_steps.index(cz % nz)]
                    return jnp.where(lane == lz - 1 - at, other, v)
                v = jnp.where(lane == at, other, v)
            if cy:
                v = rolled(v, cy, 0)
            if cz:
                v = rolled(v, cz, 1)
            return v

        def gather(x, known):
            return {q: streamed(q, x) for q in range(count_q) if (0 <= x - lattice_moves[q][0] < lx) == known}

        def advance(x, known=None):
            f = dict(known or gather(x, True))
            f.update(gather(x, False))
            result = collided([f[q] for q in range(count_q)])
            for q in range(count_q):
                out_vm[q, x] = result[q]

        def go_up():
            @each(up, order)
            def _(at):
                pl.semaphore_wait(ack_sem.at[at], 1)
                if at != last:
                    send_moments(at)

            for offset in around:
                if offset[0] or offset[1]:
                    @pl.when(me == (last - offset[0]) % nx if offset[0] else jnp.logical_not(is_lower(offset)))
                    def _():
                        pl.semaphore_wait(around_sem.at[around.index(offset)], 1)

            for sign in (-1, 1):
                @pl.when(jnp.logical_not(is_lower((sign, 0, 0))))
                def _():
                    send_face(sign)

            @pl.when(me != last)
            def _():
                send_moments(last)

            each(aside, order)(send_moments)

        go_up()
        if split_y:
            for sign in (1, -1):
                at = ly - 1 if sign > 0 else 0
                for i, q in enumerate(movers(1, sign)):
                    for x in range(lx):
                        row_y[side(sign), i, x:x + 1, :] = pop[q, x, at:at + 1, :]
            for sign in (1, -1):
                send_y(row_y.at[side(sign)], face_y.at[side(sign)], (0, sign, 0))
            for i, q in enumerate(edges_yz):
                send_y(pack_z.at[side(lattice_moves[q][2])], edge_yz.at[i], lattice_moves[q])
            for i, q in enumerate(edges_xy):
                send_y(row_y.at[side(lattice_moves[q][1]), place_in(q, 1)], edge_xy.at[i], lattice_moves[q])

        all_z.wait_recv()
        for copy in y_copies:
            copy.wait_recv()
        for x in range(1, lx - 1):
            advance(x)
        each(down - early, order[1:])(send_moments)
        known = gather(lx - 1, True)
        all_x[1].wait_recv()
        advance(lx - 1, known)
        known = gather(0, True)
        all_x[0].wait_recv()
        advance(0, known)

        for copy in all_x + [all_z, all_m] + y_copies:
            copy.wait_send()
        all_m.wait_recv()

    dma = pltpu.SemaphoreType.DMA
    y_sems = [dma((10,))] * 2 if split_y else []
    pl.run_scoped(
        scoped, dma((len(load_chunks(lx)),)), dma((4,)), dma((4,)),
        pltpu.SemaphoreType.REGULAR((nx,)), pltpu.SemaphoreType.REGULAR((len(around),)), *y_sems)


def finish(next_vm, recv_m, next_ref, slab_ref, slab_vm):
    def scoped(sems):
        store = pltpu.make_async_copy(next_vm, next_ref, sems.at[0])
        store.start()
        _, lx, ly, lz = slab_vm.shape
        for p in range(2):
            square = recv_m[:, p].reshape(lz, lz).T
            slab_vm[2 * p:2 * p + 2] = square.reshape(2, lx, ly, lz)
        slab_store = pltpu.make_async_copy(slab_vm, slab_ref, sems.at[1])
        slab_store.start()
        store.wait()
        slab_store.wait()

    pl.run_scoped(scoped, pltpu.SemaphoreType.DMA((2,)))


def on_device(axes, sizes, populations):
    q, lx, ly, lz = populations.shape
    nx, ny, nz = (sizes[a] for a in axes)
    faces = len(movers(0, 1))
    edges = 2 if nz > 2 else 1
    f32 = jnp.float32
    tile = (ly, lz)
    held = pl.pallas_call(
        functools.partial(kernel, axes, sizes),
        out_shape=(
            pltpu.VMEM(populations.shape, f32),
            pltpu.VMEM((nx, 2, lx, lz), f32),
        ),
        in_specs=[pl.BlockSpec(memory_space=pl.ANY)],
        out_specs=(pl.BlockSpec(memory_space=pltpu.VMEM),) * 2,
        scratch_shapes=[
            pltpu.VMEM(populations.shape, f32),
            pltpu.VMEM((2, faces + edges) + tile, f32),
            pltpu.VMEM((2,) + tile, f32),
            pltpu.VMEM((2, 2) + tile, f32),
            pltpu.VMEM((2,) + tile, f32),
            pltpu.VMEM((2,) + tile, f32),
            pltpu.VMEM((nx, 2, lx, lz), f32),
            pltpu.VMEM((2, 5, lx, lz), f32),
            pltpu.VMEM((2, 5, lx, lz), f32),
            pltpu.VMEM((4, lx, lz), f32),
            pltpu.VMEM((4,) + tile, f32),
        ],
        compiler_params=pltpu.CompilerParams(collective_id=0, has_side_effects=True),
        name="lattice_step",
    )(populations)
    held = [pltpu.with_memory_space_constraint(h, pltpu.VMEM) for h in held]
    slab = (4, lx, ly, lz)
    return pl.pallas_call(
        finish,
        out_shape=(jax.ShapeDtypeStruct(populations.shape, f32), jax.ShapeDtypeStruct(slab, f32)),
        in_specs=[pl.BlockSpec(memory_space=pltpu.VMEM)] * 2,
        out_specs=(pl.BlockSpec(memory_space=pl.ANY),) * 2,
        scratch_shapes=[pltpu.VMEM(slab, f32)],
        name="finish",
    )(*held)


def solution(mesh):
    axes = tuple(mesh.axis_names)
    sizes = dict(mesh.shape)
    return jax.shard_map(
        functools.partial(on_device, axes, sizes),
        mesh=mesh,
        in_specs=(P(None, "gx", "gy", "gz"),),
        out_specs=(P(None, "gx", "gy", "gz"), P(None, ("gz", "gx"), "gy", None)),
        check_vma=False,
    )
```

```python
import functools

import jax
import jax.numpy as jnp
from jax import lax
from jax.experimental import pallas as pl
from jax.experimental.pallas import tpu as pltpu
from jax.sharding import PartitionSpec as P

MESH = pl.DeviceIdType.MESH

lattice_moves = [
    (0, 0, 0),
    (1, 0, 0),
    (-1, 0, 0),
    (0, 1, 0),
    (0, -1, 0),
    (0, 0, 1),
    (0, 0, -1),
    (1, 1, 0),
    (-1, -1, 0),
    (1, -1, 0),
    (-1, 1, 0),
    (1, 0, 1),
    (-1, 0, -1),
    (1, 0, -1),
    (-1, 0, 1),
    (0, 1, 1),
    (0, -1, -1),
    (0, 1, -1),
    (0, -1, 1),
]
lattice_weights = [1.0 / 3.0] + [1.0 / 18.0] * 6 + [1.0 / 36.0] * 12
relaxation = 1.6
count_q = len(lattice_moves)


def movers(component, sign):
    return [q for q, move in enumerate(lattice_moves) if move[component] == sign]


def place_in(q, component):
    return movers(component, lattice_moves[q][component]).index(q)


def side(sign):
    return 0 if sign > 0 else 1


edges_xz = [q for q, m in enumerate(lattice_moves) if m[0] and m[2]]
edges_xy = [q for q, m in enumerate(lattice_moves) if m[0] and m[1]]
edges_yz = [q for q, m in enumerate(lattice_moves) if m[1] and m[2]]


def total(terms):
    terms = list(terms)
    while len(terms) > 1:
        terms = [
            terms[i] + terms[i + 1] if i + 1 < len(terms) else terms[i]
            for i in range(0, len(terms), 2)
        ]
    return terms[0]


def moments_of(f):
    density = total(f)
    inverse = 1.0 / density
    velocity = []
    for component in range(3):
        plus = total(f[q] for q in movers(component, 1))
        minus = total(f[q] for q in movers(component, -1))
        velocity.append((plus - minus) * inverse)
    return density, velocity


def collided(f):
    density, velocity = moments_of(f)
    speed_sq = velocity[0] * velocity[0] + velocity[1] * velocity[1] + velocity[2] * velocity[2]
    base = 1.0 - 1.5 * speed_sq
    scaled = {w: (relaxation * w) * density for w in set(lattice_weights)}
    keep = 1.0 - relaxation
    result = [None] * count_q
    result[0] = keep * f[0] + scaled[lattice_weights[0]] * base
    for q in range(1, count_q, 2):
        move = lattice_moves[q]
        projected = None
        for component in range(3):
            if move[component] == 0:
                continue
            if projected is None:
                projected = velocity[component] if move[component] > 0 else -velocity[component]
            elif move[component] > 0:
                projected = projected + velocity[component]
            else:
                projected = projected - velocity[component]
        even = base + 4.5 * (projected * projected)
        odd = 3.0 * projected
        weight = scaled[lattice_weights[q]]
        result[q] = keep * f[q] + weight * (even + odd)
        result[q + 1] = keep * f[q + 1] + weight * (even - odd)
    return result


def rolled(v, shift, axis):
    return pltpu.roll(v, shift % v.shape[axis], axis)


def digits(at):
    return at % 2, at // 2 % 2, at // 4


def entry_order(nx):
    return sorted(range(nx), key=lambda at: (sum(digits(at)), at))


def meets(low, high, nx):
    below = all(a <= b for a, b in zip(digits(low), digits(high)))
    return low != high and (below or high == entry_order(nx)[-1]) and low != entry_order(nx)[-1]


def load_chunks(lx):
    return ((lx - 1, lx), (0, lx - 1))


def kernel(axes, sizes, pop_hbm, out_vm, recv_m,
           pop, land_x, face_z, turned, pack_x, pack_z, send_m,
           row_y, face_y, edge_xy, edge_yz):
    nx, ny, nz = (sizes[a] for a in axes)
    here = tuple(lax.axis_index(a) for a in axes)
    me = here[0]
    _, lx, ly, lz = pop.shape
    split_y = ny > 1
    faces = len(movers(0, 1))
    order = entry_order(nx)
    last = order[-1]

    def device_at(offset):
        return tuple(
            lax.rem(h + o % n, n) if o % n else h
            for h, o, n in zip(here, offset, (nx, ny, nz))
        )

    def column(target):
        return (target,) + here[1:]

    def lookup(values):
        value = jnp.int32(values[0])
        for at in range(1, nx):
            value = jnp.where(me == at, values[at], value)
        return value

    def step_bits(relation):
        return lookup([
            relation(at, (at + 1) % nx) + 2 * relation(at, (at - 1) % nx) for at in range(nx)])

    beside_lower = step_bits(lambda at, t: int(meets(t, at, nx)))
    beside_higher = step_bits(lambda at, t: int(meets(at, t, nx) and t != last))

    def beside(bits, offset):
        return (bits & (1 if offset[0] % nx == 1 else 2)) != 0

    def is_lower(offset):
        if offset[0]:
            return beside(beside_lower, offset)
        _, b, c = device_at(offset)
        return b * nz + c < here[1] * nz + here[2]

    def mask(chosen):
        return lookup([sum(1 << t for t in range(nx) if chosen(at, t)) for at in range(nx)])

    offsets = [(0, 0, 1), (0, 0, -1)]
    offsets += [lattice_moves[q] for q in edges_xz]
    if split_y:
        offsets += [(0, 1, 0), (0, -1, 0)]
        offsets += [lattice_moves[q] for q in edges_xy + edges_yz]
    around = sorted({(a % nx, b % ny, c % nz) for a, b, c in offsets})

    adjacent = sorted({o[1:] for o in around if o[0]})

    def scoped(load_sem, send_sem, recv_sem, ack_sem, around_sem, *y_sems):
        loads = []
        for i, (first, end) in enumerate(load_chunks(lx)):
            planes = pl.ds(first, end - first)
            load = pltpu.make_async_copy(pop_hbm.at[:, planes], pop.at[:, planes], load_sem.at[i])
            load.start()
            loads.append(load)

        up = mask(lambda at, t: meets(at, t, nx))
        down = mask(lambda at, t: meets(t, at, nx))
        aside = mask(lambda at, t: at != t and not meets(at, t, nx) and not meets(t, at, nx))

        def each(chosen, targets):
            def run(body):
                for at in targets:
                    pl.when((chosen & (1 << at)) != 0)(functools.partial(body, at))
            return run

        barrier = pltpu.get_barrier_semaphore()
        lower = lookup([sum(meets(t, at, nx) for t in range(nx)) for at in range(nx)])

        @each(up, order)
        def _(at):
            pl.semaphore_signal(barrier, inc=1, device_id=column(at), device_id_type=MESH)

        for offset in around:
            goes = beside(beside_higher, offset) if offset[0] else jnp.logical_not(is_lower(offset))

            @pl.when(goes)
            def _():
                pl.semaphore_signal(barrier, inc=1, device_id=device_at(offset), device_id_type=MESH)

            comes = jnp.logical_and(is_lower(offset), me != last) if offset[0] else is_lower(offset)
            lower = lower + jnp.where(comes, 1, 0)
        for b, c in adjacent:
            _, there_b, there_c = device_at((0, b, c))

            @pl.when(me != last)
            def _():
                pl.semaphore_signal(
                    barrier, inc=1, device_id=(last, there_b, there_c), device_id_type=MESH)

        lower = lower + jnp.where(me == last, len(adjacent) * (nx - 1), 0)

        @pl.when(lower > 0)
        def _():
            pl.semaphore_wait(barrier, lower)

        for offset in around:
            back = tuple(-o % n for o, n in zip(offset, (nx, ny, nz)))

            @pl.when(me == last if offset[0] else is_lower(offset))
            def _():
                pl.semaphore_signal(
                    around_sem.at[around.index(back)], inc=1,
                    device_id=device_at(offset), device_id_type=MESH)

        @each(down, order)
        def _(at):
            pl.semaphore_signal(ack_sem.at[me], inc=1, device_id=column(at), device_id_type=MESH)

        lane = lax.broadcasted_iota(jnp.int32, (ly, lz), 1)
        row = lax.broadcasted_iota(jnp.int32, (ly, lz), 0)

        def remote(src, dst, kind, slot, offset):
            return pltpu.make_async_remote_copy(
                src_ref=src, dst_ref=dst, send_sem=send_sem.at[kind], recv_sem=recv_sem.at[slot],
                device_id=device_at(offset), device_id_type=MESH)

        y_copies = []

        def send_y(src, dst, offset):
            i = len(y_copies)
            copy = pltpu.make_async_remote_copy(
                src_ref=src, dst_ref=dst, send_sem=y_sems[0].at[i], recv_sem=y_sems[1].at[i],
                device_id=device_at(offset), device_id_type=MESH)
            copy.start()
            y_copies.append(copy)

        edge_steps = []
        for cz in (1, -1):
            if cz % nz not in edge_steps:
                edge_steps.append(cz % nz)

        def pack_edge(sign):
            s, at = side(sign), lx - 1 if sign > 0 else 0
            for j, cz in enumerate((1, -1)):
                turned[s, j] = rolled(pop[lattice_moves.index((sign, 0, cz)), at], cz, 1)
            pack_x[s] = jnp.where(lane == 0, turned[s, 0], turned[s, 1])

        def send_plain(sign):
            s, at = side(sign), lx - 1 if sign > 0 else 0
            for j, q in enumerate(movers(0, sign)):
                if not lattice_moves[q][2]:
                    remote(pop.at[q, at], land_x.at[s, j], s, s, (sign, 0, 0)).start()

        def send_turned(sign):
            s = side(sign)
            for j, q in enumerate(movers(0, sign)):
                if lattice_moves[q][2]:
                    i = (1, -1).index(lattice_moves[q][2])
                    remote(turned.at[s, i], land_x.at[s, j], s, s, (sign, 0, 0)).start()
            for j, cz in enumerate(edge_steps):
                remote(pack_x.at[s], land_x.at[s, faces + j], s, s, (sign, 0, cz)).start()

        def send_face(sign):
            send_plain(sign)
            send_turned(sign)

        def send_moments(target):
            pltpu.make_async_remote_copy(
                src_ref=send_m.at[target], dst_ref=recv_m.at[me],
                send_sem=send_sem.at[3], recv_sem=recv_sem.at[3],
                device_id=column(target), device_id_type=MESH).start()

        def send_z(sign):
            remote(pack_z.at[side(sign)], face_z.at[side(sign)], 2, 2, (0, 0, sign)).start()

        lane_x = lane & (lx - 1)
        values = [[None] * lx for _ in range(4)]

        def measure(x):
            density, velocity = moments_of([pop[q, x] for q in range(count_q)])
            for c, value in enumerate([density] + velocity):
                values[c][x] = value

        def skewed(tiles):
            step = 1
            while step < lx:
                odd = (lane & step) != 0
                tiles = [jnp.where(odd, tiles[(k + step) % lx], tiles[k]) for k in range(lx)]
                step *= 2
            return tiles

        def exchanged(tiles):
            tiles = skewed(tiles)
            tiles = [tiles[0]] + [
                jnp.where(lane_x >= k, rolled(tiles[k], k, 1), rolled(tiles[k], k - lx, 1))
                for k in range(1, lx)]
            tiles = skewed(tiles)
            return [tiles[-z % lx] for z in range(lx)]

        for i, (first, end) in enumerate(load_chunks(lx)):
            loads[i].wait()
            if first <= lx - 1 < end:
                @pl.when(is_lower((1, 0, 0)))
                def _():
                    send_plain(1)

                pack_edge(1)

                @pl.when(is_lower((1, 0, 0)))
                def _():
                    send_turned(1)

            for x in range(first, end):
                measure(x)

        for p in range(2):
            rows = exchanged(values[2 * p]) + exchanged(values[2 * p + 1])
            square = jnp.concatenate(rows, axis=0).T
            for j in range(nx):
                send_m[j, p] = square[j * lx:(j + 1) * lx]

        early = jnp.where(here[2] == 0, down, 0)
        each(down, order[:1])(send_moments)
        each(early, order[1:1])(send_moments)

        pack_edge(-1)

        @pl.when(is_lower((-1, 0, 0)))
        def _():
            send_face(-1)

        for sign in (1, -1):
            at = lz - 1 if sign > 0 else 0
            packed = jnp.zeros((ly, lz), jnp.float32)
            for i, q in enumerate(movers(2, sign)):
                for x in range(lx):
                    k = i * lx + x
                    packed = jnp.where(lane == k, rolled(pop[q, x], k - at, 1), packed)
            pack_z[side(sign)] = packed
        for offset in around:
            if offset[0] == offset[1] == 0:
                @pl.when(jnp.logical_not(is_lower(offset)))
                def _():
                    pl.semaphore_wait(around_sem.at[around.index(offset)], 1)
        for sign in (1, -1):
            send_z(sign)
        each(early, order[1:])(send_moments)
        recv_m[me] = send_m[me]

        all_x = [remote(land_x.at[s], land_x.at[s], s, s, (1, 0, 0)) for s in range(2)]
        all_z = remote(face_z, face_z, 2, 2, (0, 0, 1))
        others = pl.ds(0, nx - 1)
        all_m = remote(send_m.at[others], send_m.at[others], 3, 3, (1, 0, 0))

        def streamed(q, x):
            cx, cy, cz = lattice_moves[q]
            sx = x - cx
            inside = 0 <= sx < lx
            sx_wrapped = sx % lx
            v = pop[q, sx] if inside else land_x[side(cx), place_in(q, 0)]
            if cy and split_y:
                at = ly - 1 if cy > 0 else 0
                if inside:
                    other = face_y[side(cy), place_in(q, 1), sx:sx + 1, :]
                else:
                    other = edge_xy[edges_xy.index(q), sx_wrapped:sx_wrapped + 1, :]
                v = jnp.where(row == at, jnp.broadcast_to(other, v.shape), v)
            if cz:
                at = lz - 1 if cz > 0 else 0
                if inside:
                    other = face_z[side(cz)]
                    if cy and split_y:
                        at_y = ly - 1 if cy > 0 else 0
                        other = jnp.where(row == at_y, edge_yz[edges_yz.index(q)], other)
                    k = place_in(q, 2) * lx + sx
                    other = rolled(other, at - k, 1)
                else:
                    other = land_x[side(cx), faces + edge_steps.index(cz % nz)]
                    return jnp.where(lane == lz - 1 - at, other, v)
                v = jnp.where(lane == at, other, v)
            if cy:
                v = rolled(v, cy, 0)
            if cz:
                v = rolled(v, cz, 1)
            return v

        def gather(x, known):
            return {q: streamed(q, x) for q in range(count_q) if (0 <= x - lattice_moves[q][0] < lx) == known}

        def advance(x, known=None):
            f = dict(known or gather(x, True))
            f.update(gather(x, False))
            result = collided([f[q] for q in range(count_q)])
            for q in range(count_q):
                out_vm[q, x] = result[q]

        def go_up():
            @each(up, order)
            def _(at):
                pl.semaphore_wait(ack_sem.at[at], 1)
                if at != last:
                    send_moments(at)

            for offset in around:
                if offset[0] or offset[1]:
                    @pl.when(me == (last - offset[0]) % nx if offset[0] else jnp.logical_not(is_lower(offset)))
                    def _():
                        pl.semaphore_wait(around_sem.at[around.index(offset)], 1)

            each(aside, (order[4],))(send_moments)

            for sign in (-1, 1):
                @pl.when(jnp.logical_not(is_lower((sign, 0, 0))))
                def _():
                    send_face(sign)

            @pl.when(me != last)
            def _():
                send_moments(last)

            each(aside, [at for at in order if at not in (order[4],)])(send_moments)

        go_up()
        if split_y:
            for sign in (1, -1):
                at = ly - 1 if sign > 0 else 0
                for i, q in enumerate(movers(1, sign)):
                    for x in range(lx):
                        row_y[side(sign), i, x:x + 1, :] = pop[q, x, at:at + 1, :]
            for sign in (1, -1):
                send_y(row_y.at[side(sign)], face_y.at[side(sign)], (0, sign, 0))
            for i, q in enumerate(edges_yz):
                send_y(pack_z.at[side(lattice_moves[q][2])], edge_yz.at[i], lattice_moves[q])
            for i, q in enumerate(edges_xy):
                send_y(row_y.at[side(lattice_moves[q][1]), place_in(q, 1)], edge_xy.at[i], lattice_moves[q])

        all_z.wait_recv()
        for copy in y_copies:
            copy.wait_recv()
        for x in range(1, lx - 1):
            advance(x)
        each(down - early, order[1:])(send_moments)
        known = gather(lx - 1, True)
        all_x[1].wait_recv()
        advance(lx - 1, known)
        known = gather(0, True)
        all_x[0].wait_recv()
        advance(0, known)

        for copy in all_x + [all_z, all_m] + y_copies:
            copy.wait_send()
        all_m.wait_recv()

    dma = pltpu.SemaphoreType.DMA
    y_sems = [dma((10,))] * 2 if split_y else []
    pl.run_scoped(
        scoped, dma((len(load_chunks(lx)),)), dma((4,)), dma((4,)),
        pltpu.SemaphoreType.REGULAR((nx,)), pltpu.SemaphoreType.REGULAR((len(around),)), *y_sems)


def finish(next_vm, recv_m, next_ref, slab_ref, slab_vm):
    def scoped(sems):
        store = pltpu.make_async_copy(next_vm, next_ref, sems.at[0])
        store.start()
        _, lx, ly, lz = slab_vm.shape
        for p in range(2):
            square = recv_m[:, p].reshape(lz, lz).T
            slab_vm[2 * p:2 * p + 2] = square.reshape(2, lx, ly, lz)
        slab_store = pltpu.make_async_copy(slab_vm, slab_ref, sems.at[1])
        slab_store.start()
        store.wait()
        slab_store.wait()

    pl.run_scoped(scoped, pltpu.SemaphoreType.DMA((2,)))


def on_device(axes, sizes, populations):
    q, lx, ly, lz = populations.shape
    nx, ny, nz = (sizes[a] for a in axes)
    faces = len(movers(0, 1))
    edges = 2 if nz > 2 else 1
    f32 = jnp.float32
    tile = (ly, lz)
    held = pl.pallas_call(
        functools.partial(kernel, axes, sizes),
        out_shape=(
            pltpu.VMEM(populations.shape, f32),
            pltpu.VMEM((nx, 2, lx, lz), f32),
        ),
        in_specs=[pl.BlockSpec(memory_space=pl.ANY)],
        out_specs=(pl.BlockSpec(memory_space=pltpu.VMEM),) * 2,
        scratch_shapes=[
            pltpu.VMEM(populations.shape, f32),
            pltpu.VMEM((2, faces + edges) + tile, f32),
            pltpu.VMEM((2,) + tile, f32),
            pltpu.VMEM((2, 2) + tile, f32),
            pltpu.VMEM((2,) + tile, f32),
            pltpu.VMEM((2,) + tile, f32),
            pltpu.VMEM((nx, 2, lx, lz), f32),
            pltpu.VMEM((2, 5, lx, lz), f32),
            pltpu.VMEM((2, 5, lx, lz), f32),
            pltpu.VMEM((4, lx, lz), f32),
            pltpu.VMEM((4,) + tile, f32),
        ],
        compiler_params=pltpu.CompilerParams(collective_id=0, has_side_effects=True),
        name="lattice_step",
    )(populations)
    held = [pltpu.with_memory_space_constraint(h, pltpu.VMEM) for h in held]
    slab = (4, lx, ly, lz)
    return pl.pallas_call(
        finish,
        out_shape=(jax.ShapeDtypeStruct(populations.shape, f32), jax.ShapeDtypeStruct(slab, f32)),
        in_specs=[pl.BlockSpec(memory_space=pltpu.VMEM)] * 2,
        out_specs=(pl.BlockSpec(memory_space=pl.ANY),) * 2,
        scratch_shapes=[pltpu.VMEM(slab, f32)],
        name="finish",
    )(*held)


def solution(mesh):
    axes = tuple(mesh.axis_names)
    sizes = dict(mesh.shape)
    return jax.shard_map(
        functools.partial(on_device, axes, sizes),
        mesh=mesh,
        in_specs=(P(None, "gx", "gy", "gz"),),
        out_specs=(P(None, "gx", "gy", "gz"), P(None, ("gz", "gx"), "gy", None)),
        check_vma=False,
    )
```

```python
import functools

import jax
import jax.numpy as jnp
from jax import lax
from jax.experimental import pallas as pl
from jax.experimental.pallas import tpu as pltpu
from jax.sharding import PartitionSpec as P

MESH = pl.DeviceIdType.MESH

lattice_moves = [
    (0, 0, 0),
    (1, 0, 0),
    (-1, 0, 0),
    (0, 1, 0),
    (0, -1, 0),
    (0, 0, 1),
    (0, 0, -1),
    (1, 1, 0),
    (-1, -1, 0),
    (1, -1, 0),
    (-1, 1, 0),
    (1, 0, 1),
    (-1, 0, -1),
    (1, 0, -1),
    (-1, 0, 1),
    (0, 1, 1),
    (0, -1, -1),
    (0, 1, -1),
    (0, -1, 1),
]
lattice_weights = [1.0 / 3.0] + [1.0 / 18.0] * 6 + [1.0 / 36.0] * 12
relaxation = 1.6
count_q = len(lattice_moves)


def movers(component, sign):
    return [q for q, move in enumerate(lattice_moves) if move[component] == sign]


def place_in(q, component):
    return movers(component, lattice_moves[q][component]).index(q)


def side(sign):
    return 0 if sign > 0 else 1


edges_xz = [q for q, m in enumerate(lattice_moves) if m[0] and m[2]]
edges_xy = [q for q, m in enumerate(lattice_moves) if m[0] and m[1]]
edges_yz = [q for q, m in enumerate(lattice_moves) if m[1] and m[2]]


def total(terms):
    terms = list(terms)
    while len(terms) > 1:
        terms = [
            terms[i] + terms[i + 1] if i + 1 < len(terms) else terms[i]
            for i in range(0, len(terms), 2)
        ]
    return terms[0]


def moments_of(f):
    density = total(f)
    inverse = 1.0 / density
    velocity = []
    for component in range(3):
        plus = total(f[q] for q in movers(component, 1))
        minus = total(f[q] for q in movers(component, -1))
        velocity.append((plus - minus) * inverse)
    return density, velocity


def collided(f):
    density, velocity = moments_of(f)
    speed_sq = velocity[0] * velocity[0] + velocity[1] * velocity[1] + velocity[2] * velocity[2]
    base = 1.0 - 1.5 * speed_sq
    scaled = {w: (relaxation * w) * density for w in set(lattice_weights)}
    keep = 1.0 - relaxation
    result = [None] * count_q
    result[0] = keep * f[0] + scaled[lattice_weights[0]] * base
    for q in range(1, count_q, 2):
        move = lattice_moves[q]
        projected = None
        for component in range(3):
            if move[component] == 0:
                continue
            if projected is None:
                projected = velocity[component] if move[component] > 0 else -velocity[component]
            elif move[component] > 0:
                projected = projected + velocity[component]
            else:
                projected = projected - velocity[component]
        even = base + 4.5 * (projected * projected)
        odd = 3.0 * projected
        weight = scaled[lattice_weights[q]]
        result[q] = keep * f[q] + weight * (even + odd)
        result[q + 1] = keep * f[q + 1] + weight * (even - odd)
    return result


def rolled(v, shift, axis):
    return pltpu.roll(v, shift % v.shape[axis], axis)


def digits(at):
    return at % 2, at // 2 % 2, at // 4


def entry_order(nx):
    return sorted(range(nx), key=lambda at: (sum(digits(at)), at))


def meets(low, high, nx):
    below = all(a <= b for a, b in zip(digits(low), digits(high)))
    return low != high and (below or high == entry_order(nx)[-1]) and low != entry_order(nx)[-1]


def load_chunks(lx):
    return ((lx - 1, lx), (0, lx - 1))


def kernel(axes, sizes, pop_hbm, out_vm, recv_m,
           pop, land_x, face_z, turned, pack_x, pack_z, send_m,
           row_y, face_y, edge_xy, edge_yz):
    nx, ny, nz = (sizes[a] for a in axes)
    here = tuple(lax.axis_index(a) for a in axes)
    me = here[0]
    _, lx, ly, lz = pop.shape
    split_y = ny > 1
    faces = len(movers(0, 1))
    order = entry_order(nx)
    last = order[-1]

    def device_at(offset):
        return tuple(
            lax.rem(h + o % n, n) if o % n else h
            for h, o, n in zip(here, offset, (nx, ny, nz))
        )

    def column(target):
        return (target,) + here[1:]

    def lookup(values):
        value = jnp.int32(values[0])
        for at in range(1, nx):
            value = jnp.where(me == at, values[at], value)
        return value

    def step_bits(relation):
        return lookup([
            relation(at, (at + 1) % nx) + 2 * relation(at, (at - 1) % nx) for at in range(nx)])

    beside_lower = step_bits(lambda at, t: int(meets(t, at, nx)))
    beside_higher = step_bits(lambda at, t: int(meets(at, t, nx) and t != last))

    def beside(bits, offset):
        return (bits & (1 if offset[0] % nx == 1 else 2)) != 0

    def is_lower(offset):
        if offset[0]:
            return beside(beside_lower, offset)
        _, b, c = device_at(offset)
        return b * nz + c < here[1] * nz + here[2]

    def mask(chosen):
        return lookup([sum(1 << t for t in range(nx) if chosen(at, t)) for at in range(nx)])

    offsets = [(0, 0, 1), (0, 0, -1)]
    offsets += [lattice_moves[q] for q in edges_xz]
    if split_y:
        offsets += [(0, 1, 0), (0, -1, 0)]
        offsets += [lattice_moves[q] for q in edges_xy + edges_yz]
    around = sorted({(a % nx, b % ny, c % nz) for a, b, c in offsets})

    adjacent = sorted({o[1:] for o in around if o[0]})

    def scoped(load_sem, send_sem, recv_sem, ack_sem, around_sem, *y_sems):
        loads = []
        for i, (first, end) in enumerate(load_chunks(lx)):
            planes = pl.ds(first, end - first)
            load = pltpu.make_async_copy(pop_hbm.at[:, planes], pop.at[:, planes], load_sem.at[i])
            load.start()
            loads.append(load)

        up = mask(lambda at, t: meets(at, t, nx))
        down = mask(lambda at, t: meets(t, at, nx))
        aside = mask(lambda at, t: at != t and not meets(at, t, nx) and not meets(t, at, nx))

        def each(chosen, targets):
            def run(body):
                for at in targets:
                    pl.when((chosen & (1 << at)) != 0)(functools.partial(body, at))
            return run

        barrier = pltpu.get_barrier_semaphore()
        lower = lookup([sum(meets(t, at, nx) for t in range(nx)) for at in range(nx)])

        for b, c in adjacent:
            _, there_b, there_c = device_at((0, b, c))

            @pl.when(me != last)
            def _():
                pl.semaphore_signal(
                    barrier, inc=1, device_id=(last, there_b, there_c), device_id_type=MESH)

        @each(up, order[::-1])
        def _(at):
            pl.semaphore_signal(barrier, inc=1, device_id=column(at), device_id_type=MESH)

        for offset in around:
            goes = beside(beside_higher, offset) if offset[0] else jnp.logical_not(is_lower(offset))

            @pl.when(goes)
            def _():
                pl.semaphore_signal(barrier, inc=1, device_id=device_at(offset), device_id_type=MESH)

            comes = jnp.logical_and(is_lower(offset), me != last) if offset[0] else is_lower(offset)
            lower = lower + jnp.where(comes, 1, 0)
        lower = lower + jnp.where(me == last, len(adjacent) * (nx - 1), 0)

        @pl.when(lower > 0)
        def _():
            pl.semaphore_wait(barrier, lower)

        for offset in around:
            back = tuple(-o % n for o, n in zip(offset, (nx, ny, nz)))

            @pl.when(me == last if offset[0] else is_lower(offset))
            def _():
                pl.semaphore_signal(
                    around_sem.at[around.index(back)], inc=1,
                    device_id=device_at(offset), device_id_type=MESH)

        @each(down, order)
        def _(at):
            pl.semaphore_signal(ack_sem.at[me], inc=1, device_id=column(at), device_id_type=MESH)

        lane = lax.broadcasted_iota(jnp.int32, (ly, lz), 1)
        row = lax.broadcasted_iota(jnp.int32, (ly, lz), 0)

        def remote(src, dst, kind, slot, offset):
            return pltpu.make_async_remote_copy(
                src_ref=src, dst_ref=dst, send_sem=send_sem.at[kind], recv_sem=recv_sem.at[slot],
                device_id=device_at(offset), device_id_type=MESH)

        y_copies = []

        def send_y(src, dst, offset):
            i = len(y_copies)
            copy = pltpu.make_async_remote_copy(
                src_ref=src, dst_ref=dst, send_sem=y_sems[0].at[i], recv_sem=y_sems[1].at[i],
                device_id=device_at(offset), device_id_type=MESH)
            copy.start()
            y_copies.append(copy)

        edge_steps = []
        for cz in (1, -1):
            if cz % nz not in edge_steps:
                edge_steps.append(cz % nz)

        def pack_edge(sign):
            s, at = side(sign), lx - 1 if sign > 0 else 0
            for j, cz in enumerate((1, -1)):
                turned[s, j] = rolled(pop[lattice_moves.index((sign, 0, cz)), at], cz, 1)
            pack_x[s] = jnp.where(lane == 0, turned[s, 0], turned[s, 1])

        def send_plain(sign):
            s, at = side(sign), lx - 1 if sign > 0 else 0
            for j, q in enumerate(movers(0, sign)):
                if not lattice_moves[q][2]:
                    remote(pop.at[q, at], land_x.at[s, j], s, s, (sign, 0, 0)).start()

        def send_turned(sign):
            s = side(sign)
            for j, q in enumerate(movers(0, sign)):
                if lattice_moves[q][2]:
                    i = (1, -1).index(lattice_moves[q][2])
                    remote(turned.at[s, i], land_x.at[s, j], s, s, (sign, 0, 0)).start()
            for j, cz in enumerate(edge_steps):
                remote(pack_x.at[s], land_x.at[s, faces + j], s, s, (sign, 0, cz)).start()

        def send_face(sign):
            send_plain(sign)
            send_turned(sign)

        def send_moments(target):
            pltpu.make_async_remote_copy(
                src_ref=send_m.at[target], dst_ref=recv_m.at[me],
                send_sem=send_sem.at[3], recv_sem=recv_sem.at[3],
                device_id=column(target), device_id_type=MESH).start()

        def send_z(sign):
            remote(pack_z.at[side(sign)], face_z.at[side(sign)], 2, 2, (0, 0, sign)).start()

        over = row < (lane // ly) % lx
        values = [[None] * lx for _ in range(4)]

        def measure(x):
            density, velocity = moments_of([pop[q, x] for q in range(count_q)])
            for c, value in enumerate([density] + velocity):
                values[c][x] = value

        def skewed(tiles):
            step = 1
            while step < lx:
                odd = (lane & step) != 0
                tiles = [jnp.where(odd, tiles[(k + step) % lx], tiles[k]) for k in range(lx)]
                step *= 2
            return tiles

        def exchanged(tiles):
            tiles = skewed(tiles)
            tiles = [rolled(tiles[k], k, 1) if k else tiles[k] for k in range(lx)]
            tiles = skewed(tiles)
            return [tiles[-z % lx] for z in range(lx)]

        for i, (first, end) in enumerate(load_chunks(lx)):
            loads[i].wait()
            if first <= lx - 1 < end:
                @pl.when(is_lower((1, 0, 0)))
                def _():
                    send_plain(1)

                pack_edge(1)

                @pl.when(is_lower((1, 0, 0)))
                def _():
                    send_turned(1)

            for x in range(first, end):
                measure(x)

        rows = [exchanged(values[c]) for c in range(4)]
        for p in range(2):
            square = jnp.concatenate(rows[2 * p] + rows[2 * p + 1], axis=0).T
            pieces = [square[j * lx:(j + 1) * lx] for j in range(nx)]
            for j in range(nx):
                send_m[j, p] = jnp.where(over, pieces[(j + 1) % nx], pieces[j])

        early = jnp.where(here[2] == 0, down, 0)
        each(down, order[:1])(send_moments)
        each(early, order[1:1])(send_moments)

        pack_edge(-1)

        @pl.when(is_lower((-1, 0, 0)))
        def _():
            send_face(-1)

        for sign in (1, -1):
            at = lz - 1 if sign > 0 else 0
            packed = jnp.zeros((ly, lz), jnp.float32)
            for i, q in enumerate(movers(2, sign)):
                for x in range(lx):
                    k = i * lx + x
                    packed = jnp.where(lane == k, rolled(pop[q, x], k - at, 1), packed)
            pack_z[side(sign)] = packed
        for offset in around:
            if offset[0] == offset[1] == 0:
                @pl.when(jnp.logical_not(is_lower(offset)))
                def _():
                    pl.semaphore_wait(around_sem.at[around.index(offset)], 1)
        for sign in (1, -1):
            send_z(sign)
        each(early, order[1:])(send_moments)
        recv_m[me] = send_m[me]

        all_x = [remote(land_x.at[s], land_x.at[s], s, s, (1, 0, 0)) for s in range(2)]
        all_z = remote(face_z, face_z, 2, 2, (0, 0, 1))
        others = pl.ds(0, nx - 1)
        all_m = remote(send_m.at[others], send_m.at[others], 3, 3, (1, 0, 0))

        def streamed(q, x):
            cx, cy, cz = lattice_moves[q]
            sx = x - cx
            inside = 0 <= sx < lx
            sx_wrapped = sx % lx
            v = pop[q, sx] if inside else land_x[side(cx), place_in(q, 0)]
            if cy and split_y:
                at = ly - 1 if cy > 0 else 0
                if inside:
                    other = face_y[side(cy), place_in(q, 1), sx:sx + 1, :]
                else:
                    other = edge_xy[edges_xy.index(q), sx_wrapped:sx_wrapped + 1, :]
                v = jnp.where(row == at, jnp.broadcast_to(other, v.shape), v)
            if cz:
                at = lz - 1 if cz > 0 else 0
                if inside:
                    other = face_z[side(cz)]
                    if cy and split_y:
                        at_y = ly - 1 if cy > 0 else 0
                        other = jnp.where(row == at_y, edge_yz[edges_yz.index(q)], other)
                    k = place_in(q, 2) * lx + sx
                    other = rolled(other, at - k, 1)
                else:
                    other = land_x[side(cx), faces + edge_steps.index(cz % nz)]
                    return jnp.where(lane == lz - 1 - at, other, v)
                v = jnp.where(lane == at, other, v)
            if cy:
                v = rolled(v, cy, 0)
            if cz:
                v = rolled(v, cz, 1)
            return v

        def gather(x, known):
            return {q: streamed(q, x) for q in range(count_q) if (0 <= x - lattice_moves[q][0] < lx) == known}

        def advance(x, known=None):
            f = dict(known or gather(x, True))
            f.update(gather(x, False))
            result = collided([f[q] for q in range(count_q)])
            for q in range(count_q):
                out_vm[q, x] = result[q]

        def go_up():
            @each(up, order)
            def _(at):
                pl.semaphore_wait(ack_sem.at[at], 1)
                if at != last:
                    send_moments(at)

            for offset in around:
                if offset[0] or offset[1]:
                    @pl.when(me == (last - offset[0]) % nx if offset[0] else jnp.logical_not(is_lower(offset)))
                    def _():
                        pl.semaphore_wait(around_sem.at[around.index(offset)], 1)

            each(aside, (order[4],))(send_moments)

            for sign in (-1, 1):
                @pl.when(jnp.logical_not(is_lower((sign, 0, 0))))
                def _():
                    send_face(sign)

            @pl.when(me != last)
            def _():
                send_moments(last)

            each(aside, [at for at in order if at not in (order[4],)])(send_moments)

        go_up()
        if split_y:
            for sign in (1, -1):
                at = ly - 1 if sign > 0 else 0
                for i, q in enumerate(movers(1, sign)):
                    for x in range(lx):
                        row_y[side(sign), i, x:x + 1, :] = pop[q, x, at:at + 1, :]
            for sign in (1, -1):
                send_y(row_y.at[side(sign)], face_y.at[side(sign)], (0, sign, 0))
            for i, q in enumerate(edges_yz):
                send_y(pack_z.at[side(lattice_moves[q][2])], edge_yz.at[i], lattice_moves[q])
            for i, q in enumerate(edges_xy):
                send_y(row_y.at[side(lattice_moves[q][1]), place_in(q, 1)], edge_xy.at[i], lattice_moves[q])

        all_z.wait_recv()
        for copy in y_copies:
            copy.wait_recv()
        for x in range(1, lx - 1):
            advance(x)
        each(down - early, order[1:])(send_moments)
        known = gather(lx - 1, True)
        all_x[1].wait_recv()
        advance(lx - 1, known)
        known = gather(0, True)
        all_x[0].wait_recv()
        advance(0, known)

        for copy in all_x + [all_z, all_m] + y_copies:
            copy.wait_send()
        all_m.wait_recv()

    dma = pltpu.SemaphoreType.DMA
    y_sems = [dma((10,))] * 2 if split_y else []
    pl.run_scoped(
        scoped, dma((len(load_chunks(lx)),)), dma((4,)), dma((4,)),
        pltpu.SemaphoreType.REGULAR((nx,)), pltpu.SemaphoreType.REGULAR((len(around),)), *y_sems)


def finish(next_vm, recv_m, next_ref, slab_ref, slab_vm):
    def scoped(sems):
        store = pltpu.make_async_copy(next_vm, next_ref, sems.at[0])
        store.start()
        _, lx, ly, lz = slab_vm.shape
        for p in range(2):
            square = recv_m[:, p].reshape(lz, lz).T
            slab_vm[2 * p:2 * p + 2] = square.reshape(2, lx, ly, lz)
        slab_store = pltpu.make_async_copy(slab_vm, slab_ref, sems.at[1])
        slab_store.start()
        store.wait()
        slab_store.wait()

    pl.run_scoped(scoped, pltpu.SemaphoreType.DMA((2,)))


def on_device(axes, sizes, populations):
    q, lx, ly, lz = populations.shape
    nx, ny, nz = (sizes[a] for a in axes)
    faces = len(movers(0, 1))
    edges = 2 if nz > 2 else 1
    f32 = jnp.float32
    tile = (ly, lz)
    held = pl.pallas_call(
        functools.partial(kernel, axes, sizes),
        out_shape=(
            pltpu.VMEM(populations.shape, f32),
            pltpu.VMEM((nx, 2, lx, lz), f32),
        ),
        in_specs=[pl.BlockSpec(memory_space=pl.ANY)],
        out_specs=(pl.BlockSpec(memory_space=pltpu.VMEM),) * 2,
        scratch_shapes=[
            pltpu.VMEM(populations.shape, f32),
            pltpu.VMEM((2, faces + edges) + tile, f32),
            pltpu.VMEM((2,) + tile, f32),
            pltpu.VMEM((2, 2) + tile, f32),
            pltpu.VMEM((2,) + tile, f32),
            pltpu.VMEM((2,) + tile, f32),
            pltpu.VMEM((nx, 2, lx, lz), f32),
            pltpu.VMEM((2, 5, lx, lz), f32),
            pltpu.VMEM((2, 5, lx, lz), f32),
            pltpu.VMEM((4, lx, lz), f32),
            pltpu.VMEM((4,) + tile, f32),
        ],
        compiler_params=pltpu.CompilerParams(collective_id=0, has_side_effects=True),
        name="lattice_step",
    )(populations)
    held = [pltpu.with_memory_space_constraint(h, pltpu.VMEM) for h in held]
    slab = (4, lx, ly, lz)
    return pl.pallas_call(
        finish,
        out_shape=(jax.ShapeDtypeStruct(populations.shape, f32), jax.ShapeDtypeStruct(slab, f32)),
        in_specs=[pl.BlockSpec(memory_space=pltpu.VMEM)] * 2,
        out_specs=(pl.BlockSpec(memory_space=pl.ANY),) * 2,
        scratch_shapes=[pltpu.VMEM(slab, f32)],
        name="finish",
    )(*held)


def solution(mesh):
    axes = tuple(mesh.axis_names)
    sizes = dict(mesh.shape)
    return jax.shard_map(
        functools.partial(on_device, axes, sizes),
        mesh=mesh,
        in_specs=(P(None, "gx", "gy", "gz"),),
        out_specs=(P(None, "gx", "gy", "gz"), P(None, ("gz", "gx"), "gy", None)),
        check_vma=False,
    )
```

```python
import functools

import jax
import jax.numpy as jnp
from jax import lax
from jax.experimental import pallas as pl
from jax.experimental.pallas import tpu as pltpu
from jax.sharding import PartitionSpec as P

MESH = pl.DeviceIdType.MESH

lattice_moves = [
    (0, 0, 0),
    (1, 0, 0),
    (-1, 0, 0),
    (0, 1, 0),
    (0, -1, 0),
    (0, 0, 1),
    (0, 0, -1),
    (1, 1, 0),
    (-1, -1, 0),
    (1, -1, 0),
    (-1, 1, 0),
    (1, 0, 1),
    (-1, 0, -1),
    (1, 0, -1),
    (-1, 0, 1),
    (0, 1, 1),
    (0, -1, -1),
    (0, 1, -1),
    (0, -1, 1),
]
lattice_weights = [1.0 / 3.0] + [1.0 / 18.0] * 6 + [1.0 / 36.0] * 12
relaxation = 1.6
count_q = len(lattice_moves)


def movers(component, sign):
    return [q for q, move in enumerate(lattice_moves) if move[component] == sign]


def place_in(q, component):
    return movers(component, lattice_moves[q][component]).index(q)


def side(sign):
    return 0 if sign > 0 else 1


edges_xz = [q for q, m in enumerate(lattice_moves) if m[0] and m[2]]
edges_xy = [q for q, m in enumerate(lattice_moves) if m[0] and m[1]]
edges_yz = [q for q, m in enumerate(lattice_moves) if m[1] and m[2]]


def total(terms):
    terms = list(terms)
    while len(terms) > 1:
        terms = [
            terms[i] + terms[i + 1] if i + 1 < len(terms) else terms[i]
            for i in range(0, len(terms), 2)
        ]
    return terms[0]


def moments_of(f):
    density = total(f)
    inverse = 1.0 / density
    velocity = []
    for component in range(3):
        plus = total(f[q] for q in movers(component, 1))
        minus = total(f[q] for q in movers(component, -1))
        velocity.append((plus - minus) * inverse)
    return density, velocity


def collided(f):
    density, velocity = moments_of(f)
    speed_sq = velocity[0] * velocity[0] + velocity[1] * velocity[1] + velocity[2] * velocity[2]
    base = 1.0 - 1.5 * speed_sq
    scaled = {w: (relaxation * w) * density for w in set(lattice_weights)}
    keep = 1.0 - relaxation
    result = [None] * count_q
    result[0] = keep * f[0] + scaled[lattice_weights[0]] * base
    for q in range(1, count_q, 2):
        move = lattice_moves[q]
        projected = None
        for component in range(3):
            if move[component] == 0:
                continue
            if projected is None:
                projected = velocity[component] if move[component] > 0 else -velocity[component]
            elif move[component] > 0:
                projected = projected + velocity[component]
            else:
                projected = projected - velocity[component]
        even = base + 4.5 * (projected * projected)
        odd = 3.0 * projected
        weight = scaled[lattice_weights[q]]
        result[q] = keep * f[q] + weight * (even + odd)
        result[q + 1] = keep * f[q + 1] + weight * (even - odd)
    return result


def rolled(v, shift, axis):
    return pltpu.roll(v, shift % v.shape[axis], axis)


def digits(at):
    return at % 2, at // 2 % 2, at // 4


def entry_order(nx):
    return sorted(range(nx), key=lambda at: (sum(digits(at)), at))


def meets(low, high, nx):
    below = all(a <= b for a, b in zip(digits(low), digits(high)))
    return low != high and (below or high == entry_order(nx)[-1]) and low != entry_order(nx)[-1]


def load_chunks(lx):
    return ((lx - 1, lx), (0, lx - 1))


def kernel(axes, sizes, pop_hbm, out_vm, recv_m,
           pop, land_x, face_z, turned, pack_x, pack_z, send_m,
           row_y, face_y, edge_xy, edge_yz):
    nx, ny, nz = (sizes[a] for a in axes)
    here = tuple(lax.axis_index(a) for a in axes)
    me = here[0]
    _, lx, ly, lz = pop.shape
    split_y = ny > 1
    faces = len(movers(0, 1))
    order = entry_order(nx)
    last = order[-1]

    def device_at(offset):
        return tuple(
            lax.rem(h + o % n, n) if o % n else h
            for h, o, n in zip(here, offset, (nx, ny, nz))
        )

    def column(target):
        return (target,) + here[1:]

    def lookup(values):
        value = jnp.int32(values[0])
        for at in range(1, nx):
            value = jnp.where(me == at, values[at], value)
        return value

    def step_bits(relation):
        return lookup([
            relation(at, (at + 1) % nx) + 2 * relation(at, (at - 1) % nx) for at in range(nx)])

    beside_lower = step_bits(lambda at, t: int(meets(t, at, nx)))
    beside_higher = step_bits(lambda at, t: int(meets(at, t, nx) and t != last))

    def beside(bits, offset):
        return (bits & (1 if offset[0] % nx == 1 else 2)) != 0

    def is_lower(offset):
        if offset[0]:
            return beside(beside_lower, offset)
        _, b, c = device_at(offset)
        return b * nz + c < here[1] * nz + here[2]

    def mask(chosen):
        return lookup([sum(1 << t for t in range(nx) if chosen(at, t)) for at in range(nx)])

    offsets = [(0, 0, 1), (0, 0, -1)]
    offsets += [lattice_moves[q] for q in edges_xz]
    if split_y:
        offsets += [(0, 1, 0), (0, -1, 0)]
        offsets += [lattice_moves[q] for q in edges_xy + edges_yz]
    around = sorted({(a % nx, b % ny, c % nz) for a, b, c in offsets})

    adjacent = sorted({o[1:] for o in around if o[0]})

    def scoped(load_sem, send_sem, recv_sem, ack_sem, around_sem, *y_sems):
        loads = []
        for i, (first, end) in enumerate(load_chunks(lx)):
            planes = pl.ds(first, end - first)
            load = pltpu.make_async_copy(pop_hbm.at[:, planes], pop.at[:, planes], load_sem.at[i])
            load.start()
            loads.append(load)

        up = mask(lambda at, t: meets(at, t, nx))
        down = mask(lambda at, t: meets(t, at, nx))
        aside = mask(lambda at, t: at != t and not meets(at, t, nx) and not meets(t, at, nx))

        def each(chosen, targets):
            def run(body):
                for at in targets:
                    pl.when((chosen & (1 << at)) != 0)(functools.partial(body, at))
            return run

        barrier = pltpu.get_barrier_semaphore()
        lower = lookup([sum(meets(t, at, nx) for t in range(nx)) for at in range(nx)])

        for b, c in adjacent:
            _, there_b, there_c = device_at((0, b, c))

            @pl.when(me != last)
            def _():
                pl.semaphore_signal(
                    barrier, inc=1, device_id=(last, there_b, there_c), device_id_type=MESH)

        @each(up, order[::-1])
        def _(at):
            pl.semaphore_signal(barrier, inc=1, device_id=column(at), device_id_type=MESH)

        for offset in around:
            goes = beside(beside_higher, offset) if offset[0] else jnp.logical_not(is_lower(offset))

            @pl.when(goes)
            def _():
                pl.semaphore_signal(barrier, inc=1, device_id=device_at(offset), device_id_type=MESH)

            comes = jnp.logical_and(is_lower(offset), me != last) if offset[0] else is_lower(offset)
            lower = lower + jnp.where(comes, 1, 0)
        lower = lower + jnp.where(me == last, len(adjacent) * (nx - 1), 0)

        @pl.when(lower > 0)
        def _():
            pl.semaphore_wait(barrier, lower)

        for offset in around:
            back = tuple(-o % n for o, n in zip(offset, (nx, ny, nz)))

            @pl.when(me == last if offset[0] else is_lower(offset))
            def _():
                pl.semaphore_signal(
                    around_sem.at[around.index(back)], inc=1,
                    device_id=device_at(offset), device_id_type=MESH)

        @each(down, order)
        def _(at):
            pl.semaphore_signal(ack_sem.at[me], inc=1, device_id=column(at), device_id_type=MESH)

        lane = lax.broadcasted_iota(jnp.int32, (ly, lz), 1)
        row = lax.broadcasted_iota(jnp.int32, (ly, lz), 0)

        def remote(src, dst, kind, slot, offset):
            return pltpu.make_async_remote_copy(
                src_ref=src, dst_ref=dst, send_sem=send_sem.at[kind], recv_sem=recv_sem.at[slot],
                device_id=device_at(offset), device_id_type=MESH)

        y_copies = []

        def send_y(src, dst, offset):
            i = len(y_copies)
            copy = pltpu.make_async_remote_copy(
                src_ref=src, dst_ref=dst, send_sem=y_sems[0].at[i], recv_sem=y_sems[1].at[i],
                device_id=device_at(offset), device_id_type=MESH)
            copy.start()
            y_copies.append(copy)

        edge_steps = []
        for cz in (1, -1):
            if cz % nz not in edge_steps:
                edge_steps.append(cz % nz)

        def pack_edge(sign):
            s, at = side(sign), lx - 1 if sign > 0 else 0
            for j, cz in enumerate((1, -1)):
                turned[s, j] = rolled(pop[lattice_moves.index((sign, 0, cz)), at], cz, 1)
            pack_x[s] = jnp.where(lane == 0, turned[s, 0], turned[s, 1])

        def send_plain(sign):
            s, at = side(sign), lx - 1 if sign > 0 else 0
            for j, q in enumerate(movers(0, sign)):
                if not lattice_moves[q][2]:
                    remote(pop.at[q, at], land_x.at[s, j], s, s, (sign, 0, 0)).start()

        def send_turned(sign):
            s = side(sign)
            for j, q in enumerate(movers(0, sign)):
                if lattice_moves[q][2]:
                    i = (1, -1).index(lattice_moves[q][2])
                    remote(turned.at[s, i], land_x.at[s, j], s, s, (sign, 0, 0)).start()
            for j, cz in enumerate(edge_steps):
                remote(pack_x.at[s], land_x.at[s, faces + j], s, s, (sign, 0, cz)).start()

        def send_face(sign):
            send_plain(sign)
            send_turned(sign)

        def send_moments(target):
            pltpu.make_async_remote_copy(
                src_ref=send_m.at[target], dst_ref=recv_m.at[me],
                send_sem=send_sem.at[3], recv_sem=recv_sem.at[3],
                device_id=column(target), device_id_type=MESH).start()

        def send_z(sign):
            remote(pack_z.at[side(sign)], face_z.at[side(sign)], 2, 2, (0, 0, sign)).start()

        over = row < (lane // ly) % lx
        values = [[None] * lx for _ in range(4)]

        def measure(x):
            density, velocity = moments_of([pop[q, x] for q in range(count_q)])
            for c, value in enumerate([density] + velocity):
                values[c][x] = value

        def skewed(tiles):
            step = 1
            while step < lx:
                odd = (lane & step) != 0
                tiles = [jnp.where(odd, tiles[(k + step) % lx], tiles[k]) for k in range(lx)]
                step *= 2
            return tiles

        def exchanged(tiles):
            tiles = skewed(tiles)
            tiles = [rolled(tiles[k], k, 1) if k else tiles[k] for k in range(lx)]
            tiles = skewed(tiles)
            return [tiles[-z % lx] for z in range(lx)]

        for i, (first, end) in enumerate(load_chunks(lx)):
            loads[i].wait()
            if first <= lx - 1 < end:
                @pl.when(is_lower((1, 0, 0)) & (here[2] == 0))
                def _():
                    send_plain(1)

                pack_edge(1)

                @pl.when(is_lower((1, 0, 0)) & (here[2] == 0))
                def _():
                    send_turned(1)

            for x in range(first, end):
                measure(x)

        rows = [exchanged(values[c]) for c in range(4)]
        for p in range(2):
            square = jnp.concatenate(rows[2 * p] + rows[2 * p + 1], axis=0).T
            pieces = [square[j * lx:(j + 1) * lx] for j in range(nx)]
            for j in range(nx):
                send_m[j, p] = jnp.where(over, pieces[(j + 1) % nx], pieces[j])

        early = jnp.where(here[2] == 0, down, 0)
        each(down, order[:1])(send_moments)

        @pl.when(is_lower((1, 0, 0)) & (here[2] != 0))
        def _():
            send_face(1)

        each(early, order[1:1])(send_moments)

        pack_edge(-1)

        @pl.when(is_lower((-1, 0, 0)))
        def _():
            send_face(-1)

        for sign in (1, -1):
            at = lz - 1 if sign > 0 else 0
            packed = jnp.zeros((ly, lz), jnp.float32)
            for i, q in enumerate(movers(2, sign)):
                for x in range(lx):
                    k = i * lx + x
                    packed = jnp.where(lane == k, rolled(pop[q, x], k - at, 1), packed)
            pack_z[side(sign)] = packed
        for offset in around:
            if offset[0] == offset[1] == 0:
                @pl.when(jnp.logical_not(is_lower(offset)))
                def _():
                    pl.semaphore_wait(around_sem.at[around.index(offset)], 1)
        for sign in (1, -1):
            send_z(sign)
        each(early, order[1:])(send_moments)
        recv_m[me] = send_m[me]

        all_x = [remote(land_x.at[s], land_x.at[s], s, s, (1, 0, 0)) for s in range(2)]
        all_z = remote(face_z, face_z, 2, 2, (0, 0, 1))
        others = pl.ds(0, nx - 1)
        all_m = remote(send_m.at[others], send_m.at[others], 3, 3, (1, 0, 0))

        def streamed(q, x):
            cx, cy, cz = lattice_moves[q]
            sx = x - cx
            inside = 0 <= sx < lx
            sx_wrapped = sx % lx
            v = pop[q, sx] if inside else land_x[side(cx), place_in(q, 0)]
            if cy and split_y:
                at = ly - 1 if cy > 0 else 0
                if inside:
                    other = face_y[side(cy), place_in(q, 1), sx:sx + 1, :]
                else:
                    other = edge_xy[edges_xy.index(q), sx_wrapped:sx_wrapped + 1, :]
                v = jnp.where(row == at, jnp.broadcast_to(other, v.shape), v)
            if cz:
                at = lz - 1 if cz > 0 else 0
                if inside:
                    other = face_z[side(cz)]
                    if cy and split_y:
                        at_y = ly - 1 if cy > 0 else 0
                        other = jnp.where(row == at_y, edge_yz[edges_yz.index(q)], other)
                    k = place_in(q, 2) * lx + sx
                    other = rolled(other, at - k, 1)
                else:
                    other = land_x[side(cx), faces + edge_steps.index(cz % nz)]
                    return jnp.where(lane == lz - 1 - at, other, v)
                v = jnp.where(lane == at, other, v)
            if cy:
                v = rolled(v, cy, 0)
            if cz:
                v = rolled(v, cz, 1)
            return v

        def gather(x, known):
            return {q: streamed(q, x) for q in range(count_q) if (0 <= x - lattice_moves[q][0] < lx) == known}

        def advance(x, known=None):
            f = dict(known or gather(x, True))
            f.update(gather(x, False))
            result = collided([f[q] for q in range(count_q)])
            for q in range(count_q):
                out_vm[q, x] = result[q]

        def go_up():
            @each(up, order)
            def _(at):
                pl.semaphore_wait(ack_sem.at[at], 1)
                if at != last:
                    send_moments(at)

            for offset in around:
                if offset[0] or offset[1]:
                    @pl.when(me == (last - offset[0]) % nx if offset[0] else jnp.logical_not(is_lower(offset)))
                    def _():
                        pl.semaphore_wait(around_sem.at[around.index(offset)], 1)

            each(aside, order[4:5])(send_moments)

            for sign in (-1, 1):
                @pl.when(jnp.logical_not(is_lower((sign, 0, 0))))
                def _():
                    send_face(sign)

            @pl.when(me != last)
            def _():
                send_moments(last)

            each(aside, [at for at in order if at not in order[4:5]])(send_moments)

        go_up()
        if split_y:
            for sign in (1, -1):
                at = ly - 1 if sign > 0 else 0
                for i, q in enumerate(movers(1, sign)):
                    for x in range(lx):
                        row_y[side(sign), i, x:x + 1, :] = pop[q, x, at:at + 1, :]
            for sign in (1, -1):
                send_y(row_y.at[side(sign)], face_y.at[side(sign)], (0, sign, 0))
            for i, q in enumerate(edges_yz):
                send_y(pack_z.at[side(lattice_moves[q][2])], edge_yz.at[i], lattice_moves[q])
            for i, q in enumerate(edges_xy):
                send_y(row_y.at[side(lattice_moves[q][1]), place_in(q, 1)], edge_xy.at[i], lattice_moves[q])

        all_z.wait_recv()
        for copy in y_copies:
            copy.wait_recv()
        for x in range(1, lx - 1):
            advance(x)
        each(down - early, order[1:])(send_moments)
        known = gather(lx - 1, True)
        all_x[1].wait_recv()
        advance(lx - 1, known)
        known = gather(0, True)
        all_x[0].wait_recv()
        advance(0, known)

        for copy in all_x + [all_z, all_m] + y_copies:
            copy.wait_send()
        all_m.wait_recv()

    dma = pltpu.SemaphoreType.DMA
    y_sems = [dma((10,))] * 2 if split_y else []
    pl.run_scoped(
        scoped, dma((len(load_chunks(lx)),)), dma((4,)), dma((4,)),
        pltpu.SemaphoreType.REGULAR((nx,)), pltpu.SemaphoreType.REGULAR((len(around),)), *y_sems)


def finish(next_vm, recv_m, next_ref, slab_ref, slab_vm):
    def scoped(sems):
        store = pltpu.make_async_copy(next_vm, next_ref, sems.at[0])
        store.start()
        _, lx, ly, lz = slab_vm.shape
        for p in range(2):
            square = recv_m[:, p].reshape(lz, lz).T
            slab_vm[2 * p:2 * p + 2] = square.reshape(2, lx, ly, lz)
        slab_store = pltpu.make_async_copy(slab_vm, slab_ref, sems.at[1])
        slab_store.start()
        store.wait()
        slab_store.wait()

    pl.run_scoped(scoped, pltpu.SemaphoreType.DMA((2,)))


def on_device(axes, sizes, populations):
    q, lx, ly, lz = populations.shape
    nx, ny, nz = (sizes[a] for a in axes)
    faces = len(movers(0, 1))
    edges = 2 if nz > 2 else 1
    f32 = jnp.float32
    tile = (ly, lz)
    held = pl.pallas_call(
        functools.partial(kernel, axes, sizes),
        out_shape=(
            pltpu.VMEM(populations.shape, f32),
            pltpu.VMEM((nx, 2, lx, lz), f32),
        ),
        in_specs=[pl.BlockSpec(memory_space=pl.ANY)],
        out_specs=(pl.BlockSpec(memory_space=pltpu.VMEM),) * 2,
        scratch_shapes=[
            pltpu.VMEM(populations.shape, f32),
            pltpu.VMEM((2, faces + edges) + tile, f32),
            pltpu.VMEM((2,) + tile, f32),
            pltpu.VMEM((2, 2) + tile, f32),
            pltpu.VMEM((2,) + tile, f32),
            pltpu.VMEM((2,) + tile, f32),
            pltpu.VMEM((nx, 2, lx, lz), f32),
            pltpu.VMEM((2, 5, lx, lz), f32),
            pltpu.VMEM((2, 5, lx, lz), f32),
            pltpu.VMEM((4, lx, lz), f32),
            pltpu.VMEM((4,) + tile, f32),
        ],
        compiler_params=pltpu.CompilerParams(collective_id=0, has_side_effects=True),
        name="lattice_step",
    )(populations)
    held = [pltpu.with_memory_space_constraint(h, pltpu.VMEM) for h in held]
    slab = (4, lx, ly, lz)
    return pl.pallas_call(
        finish,
        out_shape=(jax.ShapeDtypeStruct(populations.shape, f32), jax.ShapeDtypeStruct(slab, f32)),
        in_specs=[pl.BlockSpec(memory_space=pltpu.VMEM)] * 2,
        out_specs=(pl.BlockSpec(memory_space=pl.ANY),) * 2,
        scratch_shapes=[pltpu.VMEM(slab, f32)],
        name="finish",
    )(*held)


def solution(mesh):
    axes = tuple(mesh.axis_names)
    sizes = dict(mesh.shape)
    return jax.shard_map(
        functools.partial(on_device, axes, sizes),
        mesh=mesh,
        in_specs=(P(None, "gx", "gy", "gz"),),
        out_specs=(P(None, "gx", "gy", "gz"), P(None, ("gz", "gx"), "gy", None)),
        check_vma=False,
    )
```
